16 devices in a mesh: dp: 2 (over y, z), tp: 8 (over x, core).
Axes of the slice: x: 4, y: 2, z: 1, core: 2. Of those that a mesh axis runs over, the one named last changes fastest.
The devices are a block of a 4x4x8 slice.
Arguments:
- hidden: bfloat16 [4096, 512], P(('dp', 'tp')), parts along dimension 0
- ln_gain: float32 [512], replicated
- ln_bias: float32 [512], replicated
- out_embed: bfloat16 [32768, 512], P('tp')
- vocab_valid: int32 [32768], P('tp')
- targets: int32 [4096], P(('dp', 'tp')), parts along dimension 0
- loss_mask: int32 [4096], P(('dp', 'tp')), parts along dimension 0
Outputs:
- output 1: float32 [4096], P(('dp', 'tp')), parts along dimension 0
- output 2: float32 [2], P('dp'), parts along dimension 0
- output 3: bfloat16 [4096, 512], P(('dp', 'tp')), parts along dimension 0
- output 4: float32 [65536, 512], P(('dp', 'tp')), parts along dimension 0
- output 5: float32 [1024], P('dp'), parts along dimension 0
- output 6: float32 [1024], P('dp'), parts along dimension 0
There are 2 independent parts. The reference program is written for one: setup_inputs(seed, part) draws one part's arguments, and reference() takes and returns one part's arrays. A program takes and returns all parts, laid end to end along the dimension named above; an argument that names none is the same for every part.
All inputs are finite; a program needn't handle non-finite values.
Results may differ from the reference program's by a relative error of at most 0.001.
Values are sent between devices in bfloat16 or wider.
A program may use at most 768 MiB of HBM per device.

```python
import jax
import jax.numpy as jnp
from jax import lax

MODEL_DIM = 512
VOCAB_REAL = 32128
VOCAB_PAD = 32768
SEQ_LEN = 2048
TOK_BLOCK = 256
BLOCK_COUNT = SEQ_LEN // TOK_BLOCK
SOFT_CAP = 30.0
Z_COEF = 1e-4
LN_EPS = 1e-5


def layer_norm(h_float, ln_gain, ln_bias):
    mean_val = jnp.mean(h_float, axis=-1, keepdims=True)
    centered = h_float - mean_val
    var_val = jnp.mean(centered * centered, axis=-1, keepdims=True)
    return centered * lax.rsqrt(var_val + LN_EPS) * ln_gain + ln_bias


def draw_layout(shared_key, part_key):
    col_idx = jnp.arange(VOCAB_PAD)
    coin_draw = jax.random.randint(shared_key, (VOCAB_PAD,), 0, 8)
    dropped = (col_idx % 2 == 0) & (coin_draw == 0) & (col_idx < VOCAB_REAL - 1)
    vocab_valid = ((col_idx < VOCAB_REAL) & jnp.logical_not(dropped)).astype(jnp.int32)
    key_tgt, key_pre, key_post, key_hole = jax.random.split(part_key, 4)
    raw_tgt = jax.random.randint(key_tgt, (SEQ_LEN,), 0, VOCAB_REAL)
    targets = raw_tgt + 1 - vocab_valid[raw_tgt]
    positions = jnp.arange(SEQ_LEN)
    prefix_len = jax.random.randint(key_pre, (), 0, SEQ_LEN // 4 + 1)
    suffix_len = jax.random.randint(key_post, (), 0, SEQ_LEN // 4 + 1)
    hole_draw = jax.random.randint(key_hole, (SEQ_LEN,), 0, 8)
    keep_tok = (positions >= prefix_len) & (positions < SEQ_LEN - suffix_len) & (hole_draw != 0)
    keep_tok = keep_tok | (positions == SEQ_LEN // 2)
    return vocab_valid, targets.astype(jnp.int32), keep_tok.astype(jnp.int32)


def setup_inputs(seed: int = 0, part: int = 0) -> dict:
    shared_key = jax.random.key(seed)
    part_key = jax.random.fold_in(jax.random.key(seed + 1), part)
    key_gain, key_bias, key_embed, key_valid = jax.random.split(shared_key, 4)
    key_hidden, key_layout = jax.random.split(part_key, 2)
    hidden = 1.5 * jax.random.normal(key_hidden, (SEQ_LEN, MODEL_DIM), jnp.float32)
    ln_gain = 1.0 + 0.3 * jax.random.normal(key_gain, (MODEL_DIM,), jnp.float32)
    ln_bias = 0.3 * jax.random.normal(key_bias, (MODEL_DIM,), jnp.float32)
    out_embed = (3.0 * MODEL_DIM ** -0.5) * jax.random.normal(key_embed, (VOCAB_PAD, MODEL_DIM), jnp.float32)
    vocab_valid, targets, loss_mask = draw_layout(key_valid, key_layout)
    return {"hidden": hidden.astype(jnp.bfloat16), "ln_gain": ln_gain, "ln_bias": ln_bias, "out_embed": out_embed.astype(jnp.bfloat16), "vocab_valid": vocab_valid, "targets": targets, "loss_mask": loss_mask}


def reference(hidden, ln_gain, ln_bias, out_embed, vocab_valid, targets, loss_mask):
    normed, ln_back = jax.vjp(layer_norm, hidden.astype(jnp.float32), ln_gain, ln_bias)
    x_all = normed.astype(jnp.bfloat16)
    mask_f = loss_mask.astype(jnp.float32)
    tok_count = jnp.sum(mask_f)
    col_ok = (vocab_valid != 0)[None, :]
    col_ids = jnp.arange(VOCAB_PAD)[None, :]

    def block_step(embed_grad, blk_data):
        x_blk, tgt_blk, mask_blk = blk_data
        logits = jnp.dot(x_blk, out_embed.T, preferred_element_type=jnp.float32)
        tanh_val = jnp.tanh(logits / SOFT_CAP)
        capped = SOFT_CAP * tanh_val
        masked = jnp.where(col_ok, capped, -SOFT_CAP)
        row_max = jnp.max(masked, axis=1, keepdims=True)
        exp_vals = jnp.where(col_ok, jnp.exp(masked - row_max), 0.0)
        sum_exp = jnp.sum(exp_vals, axis=1, keepdims=True)
        lse = row_max[:, 0] + jnp.log(sum_exp[:, 0])
        is_target = tgt_blk[:, None] == col_ids
        tgt_logit = jnp.sum(jnp.where(is_target, capped, 0.0), axis=1)
        tok_loss = (lse - tgt_logit + Z_COEF * lse * lse) * mask_blk
        tok_coef = mask_blk / tok_count
        d_capped = ((1.0 + 2.0 * Z_COEF * lse) * tok_coef)[:, None] * (exp_vals / sum_exp) - jnp.where(is_target, tok_coef[:, None], 0.0)
        d_logits = (d_capped * (1.0 - tanh_val * tanh_val)).astype(jnp.bfloat16)
        new_grad = embed_grad + jnp.dot(d_logits.T, x_blk, preferred_element_type=jnp.float32)
        d_normed = jnp.dot(d_logits, out_embed, preferred_element_type=jnp.float32)
        return new_grad, (tok_loss, d_normed)

    init_grad = jnp.zeros((VOCAB_PAD, MODEL_DIM), jnp.float32)
    blk_inputs = (x_all.reshape(BLOCK_COUNT, TOK_BLOCK, MODEL_DIM), targets.reshape(BLOCK_COUNT, TOK_BLOCK), mask_f.reshape(BLOCK_COUNT, TOK_BLOCK))
    d_embed, (tok_loss, d_normed) = lax.scan(block_step, init_grad, blk_inputs)
    tok_loss = tok_loss.reshape(SEQ_LEN)
    d_normed = d_normed.reshape(SEQ_LEN, MODEL_DIM)
    mean_loss = jnp.sum(tok_loss) / tok_count
    d_hidden, d_gain, d_bias = ln_back(d_normed)
    return tok_loss, mean_loss.reshape(1), d_hidden.astype(jnp.bfloat16), d_embed, d_gain, d_bias
```

```python
import functools

import jax
import jax.numpy as jnp
from jax import lax
from jax.experimental import pallas as pl
from jax.experimental.pallas import tpu as pltpu
from jax.sharding import PartitionSpec as P

SOFT_CAP = 30.0
Z_COEF = 1e-4
LN_EPS = 1e-5
EXP_SCALE = SOFT_CAP * 1.4426950408889634
MESH = pl.DeviceIdType.MESH
CHIPS = 4
OFFSET = (0, 1, 3, 2)
OWN, RIGHT, LEFT, OPP = range(4)
HT = 128
SUB = 32

TO_PARTNER, TO_RIGHT, TO_LEFT, FWD_RIGHT, FWD_LEFT, REL_LEFT, REL_RIGHT, REL_OPP_A, REL_OPP_B = range(9)
PAIR, OPP_RIGHT, OPP_LEFT, RIGHT_HI, RIGHT_LO, LEFT_LO, LEFT_HI = 0, 4, 5, 6, 7, 8, 9


def norm(h):
    mean = jnp.mean(h, axis=-1, keepdims=True)
    cent = h - mean
    rstd = lax.rsqrt(jnp.mean(cent * cent, axis=-1, keepdims=True) + LN_EPS)
    return cent * rstd, rstd


def kernel(
    hid, gain, bias, e_hbm, valid, tgt, msk,
    loss_out, mean_out, dh_out, de_hbm, gb_out,
    x_all, xt, e, et, vb, w, dz, tm_all, st_send, st_recv, av, dv, ls, dx, d2d, ring, fin, gb_send, gb_recv, stage,
    e_sem, out_sem, tm_s, tm_r, ag_s, ag_r, st_s, st_r, rs_s, rs_r, gb_s, gb_r,
    *, vc, ec,
):
    group = 2 * CHIPS
    me = lax.axis_index("tp")
    c, k = me // 2, me % 2
    other = 1 - k
    partner = 2 * c + other
    chip = [(c + o) % CHIPS for o in OFFSET]
    right, left = 2 * chip[RIGHT] + k, 2 * chip[LEFT] + k
    vocab, dim = e_hbm.shape
    nv, ne = vocab // vc, vocab // ec

    def remote(src, dst, send, recv, dev):
        return pltpu.make_async_remote_copy(
            src_ref=src, dst_ref=dst, send_sem=send, recv_sem=recv, device_id={"tp": dev}, device_id_type=MESH
        )

    e_copies = [
        pltpu.make_async_copy(e_hbm.at[pl.ds(i * vc, vc)], e.at[pl.ds(i * vc, vc)], e_sem.at[i]) for i in range(nv)
    ]
    for cp in e_copies:
        cp.start()

    barrier = pltpu.get_barrier_semaphore()
    for j in range(1, group):
        pl.semaphore_signal(barrier, inc=1, device_id={"tp": (me + j) % group}, device_id_type=MESH)

    for h in range(2):
        xh, _ = norm(hid[h * HT : (h + 1) * HT, :].astype(jnp.float32))
        x_all[h, c, k] = (xh * gain[...] + bias[...]).astype(jnp.bfloat16)
    tm_all[me] = tgt[...] * 2 + msk[...]

    pl.semaphore_wait(barrier, group - 1)

    def ag(h, i, src, dst, dev):
        return remote(src, dst, ag_s.at[h * 9 + i], ag_r.at[h * 9 + i], dev)

    def lo(ref):
        return ref.at[pl.ds(0, HT // 2)]

    def hi(ref):
        return ref.at[pl.ds(HT // 2, HT // 2)]

    def block(h, r, core):
        return x_all.at[h, chip[r], core]

    def ag_copy(h, i):
        mine, lft, rgt, opp = block(h, OWN, k), block(h, LEFT, k), block(h, RIGHT, k), block(h, OPP, k)
        src, dev = {
            TO_PARTNER: (mine, partner),
            TO_RIGHT: (mine, right),
            TO_LEFT: (mine, left),
            FWD_RIGHT: (lo(lft), right),
            FWD_LEFT: (hi(rgt), left),
            REL_LEFT: (lft, partner),
            REL_RIGHT: (rgt, partner),
            REL_OPP_A: (lo(opp), partner),
            REL_OPP_B: (hi(opp), partner),
        }[i]
        return ag(h, i, src, src, dev)

    def ag_arrival(h, i):
        ref = {
            TO_PARTNER: block(h, OWN, other),
            TO_RIGHT: block(h, LEFT, k),
            TO_LEFT: block(h, RIGHT, k),
            FWD_RIGHT: lo(block(h, OPP, k)),
            FWD_LEFT: hi(block(h, OPP, k)),
            REL_LEFT: block(h, LEFT, other),
            REL_RIGHT: block(h, RIGHT, other),
            REL_OPP_A: lo(block(h, OPP, other)),
            REL_OPP_B: hi(block(h, OPP, other)),
        }[i]
        ag(h, i, ref, ref, partner).wait_recv()

    started = []

    def go(copy):
        copy.start()
        started.append(copy)

    def tm_copy(j):
        return remote(tm_all.at[me], tm_all.at[me], tm_s.at[j - 1], tm_r.at[j - 1], (me + j) % group)

    for h in range(2):
        if h == 0:
            for j in range(1, group):
                go(tm_copy(j))
        for i in (TO_PARTNER, TO_RIGHT, TO_LEFT):
            go(ag_copy(h, i))

    def tm_arrival(j):
        ref = tm_all.at[(me - j + group) % group]
        remote(ref, ref, tm_s.at[j - 1], tm_r.at[j - 1], partner).wait_recv()

    @pl.loop(0, vocab // 128)
    def _(i):
        row = jnp.broadcast_to(valid[pl.ds(i, 1), :].astype(jnp.float32), (128, 128))
        vb[pl.ds(pl.multiple_of(i * 128, 128), 128), :] = row.T

    for cp in e_copies:
        cp.wait()

    iota = lax.broadcasted_iota(jnp.int32, (SUB, 256), 0).reshape(SUB // 8, 8, 256)

    def local_target(h, chip_no):
        halves = [
            jnp.broadcast_to((tm_all[2 * chip_no + kk, pl.ds(h, 1), :] >> 1) - me * vocab, (8, 128)) for kk in range(2)
        ]
        return jnp.concatenate(halves, axis=1)

    def forward(h, r, slot):
        chip_no = chip[r]
        xt[...] = x_all[h, chip_no].reshape(2 * HT, dim).T
        tgt8 = local_target(h, chip_no)

        def body(i, carry):
            s_acc, t_acc = carry
            rows0 = pl.multiple_of(i * vc, vc)
            z = jnp.dot(e[pl.ds(rows0, vc), :], xt[...], preferred_element_type=jnp.float32)
            tgt_rel = tgt8 - rows0
            for j in range(vc // SUB):
                rows = pl.ds(pl.multiple_of(rows0 + j * SUB, SUB), SUB)
                ok = vb[rows, :]
                ok = jnp.concatenate([ok, ok], axis=1)
                t = jnp.tanh(z[j * SUB : (j + 1) * SUB, :] * (1.0 / SOFT_CAP))
                ex = jnp.exp2(t * EXP_SCALE) * ok
                w[slot, rows, :] = ex * (1.0 - t * t)
                hit = iota == (tgt_rel - j * SUB)[None]
                s_acc = s_acc + jnp.sum(ex.reshape(SUB // 8, 8, 256), axis=0)
                t_acc = t_acc + jnp.sum(jnp.where(hit, t.reshape(SUB // 8, 8, 256), 0.0), axis=0)
            return s_acc, t_acc

        zero = jnp.zeros((8, 256), jnp.float32)
        s_acc, t_acc = lax.fori_loop(0, nv, body, (zero, zero))
        s_row = jnp.sum(s_acc, axis=0, keepdims=True)
        t_row = jnp.sum(t_acc, axis=0, keepdims=True)
        for kk in range(2):
            st_send[h, pl.ds(2 * chip_no + kk, 1), :] = s_row[:, kk * 128 : (kk + 1) * 128]
            st_send[h, pl.ds(group + 2 * chip_no + kk, 1), :] = t_row[:, kk * 128 : (kk + 1) * 128]

    def st_copy(h, j):
        n = h * (group - 1) + j - 1
        return remote(st_send.at[h], st_recv.at[h, j - 1], st_s.at[n], st_r.at[n], (me + j) % group)

    def stats_start(h):
        for j in range(1, group):
            go(st_copy(h, j))

    def token_count():
        total = jnp.zeros((2, 128), jnp.int32)
        for p in range(group):
            total = total + (tm_all[p] & 1)
        total = jnp.sum(jnp.sum(total.astype(jnp.float32), axis=1, keepdims=True), axis=0, keepdims=True)
        return total

    def stats_finish(h):
        tot = st_send[h]
        for j in range(1, group):
            st_copy(h, j).wait_recv()
        for j in range(1, group):
            tot = tot + st_recv[h, j - 1]
        s, t = tot[:group], tot[group:]
        mask = jnp.concatenate([tm_all[p, pl.ds(h, 1), :] & 1 for p in range(group)], axis=0).astype(jnp.float32)
        lse = jnp.log(s)
        coef = mask / token_count()
        a = (1.0 + 2.0 * Z_COEF * lse) * coef / s
        av[h] = a
        dv[h] = (a * jnp.exp2(t * EXP_SCALE) - coef) * (1.0 - t * t)
        ls[h] = (lse - SOFT_CAP * t + Z_COEF * lse * lse) * mask

    def spread(ref, h, chip_no):
        return jnp.concatenate(
            [jnp.broadcast_to(ref[h, pl.ds(2 * chip_no + kk, 1), :], (8, 128)) for kk in range(2)], axis=1
        )

    def backward(h, r, slot):
        chip_no = chip[r]
        tile = h * CHIPS + chip_no
        tgt8 = local_target(h, chip_no)
        a8, d8 = spread(av, h, chip_no)[None], spread(dv, h, chip_no)[None]
        for kk in range(2):
            dx[h, r, kk] = jnp.zeros((dim, HT), jnp.float32)

        @pl.loop(0, nv)
        def _(i):
            rows0 = pl.multiple_of(i * vc, vc)
            tgt_rel = tgt8 - rows0
            pieces = []
            for j in range(vc // SUB):
                rows = pl.ds(pl.multiple_of(rows0 + j * SUB, SUB), SUB)
                hit = iota == (tgt_rel - j * SUB)[None]
                g = jnp.where(hit, d8, a8 * w[slot, rows, :].reshape(SUB // 8, 8, 256))
                g = g.reshape(SUB, 256).astype(jnp.bfloat16)
                dz[tile, rows, :] = g
                pieces.append(g)
            part = jnp.dot(et[i], jnp.concatenate(pieces, axis=0), preferred_element_type=jnp.float32)
            for kk in range(2):
                dx[h, r, kk] += part[:, kk * HT : (kk + 1) * HT]

    dlo, dhi = pl.ds(0, dim // 2), pl.ds(dim // 2, dim // 2)

    def rs(h, i, src, dst, dev):
        return remote(src, dst, rs_s.at[h * 10 + i], rs_r.at[h * 10 + i], dev)

    def pair_start(h, r):
        go(rs(h, PAIR + r, dx.at[h, r, other], d2d.at[h, r], partner))

    def pair_finish(h, r):
        rs(h, PAIR + r, d2d.at[h, r], d2d.at[h, r], partner).wait_recv()
        dx[h, r, k] = dx[h, r, k] + d2d[h, r]

    def opp_send(h):
        pair_finish(h, OPP)
        go(rs(h, OPP_RIGHT, dx.at[h, OPP, k, dlo], ring.at[h, 0], right))
        go(rs(h, OPP_LEFT, dx.at[h, OPP, k, dhi], ring.at[h, 1], left))

    def right_send(h):
        pair_finish(h, RIGHT)
        go(rs(h, RIGHT_HI, dx.at[h, RIGHT, k, dhi], fin.at[h, 0, dhi], right))

    def left_send(h):
        pair_finish(h, LEFT)
        go(rs(h, LEFT_LO, dx.at[h, LEFT, k, dlo], fin.at[h, 1, dlo], left))

    def ring_send(h):
        rs(h, OPP_RIGHT, ring.at[h, 0], ring.at[h, 0], partner).wait_recv()
        dx[h, RIGHT, k, dlo] = dx[h, RIGHT, k, dlo] + ring[h, 0]
        go(rs(h, RIGHT_LO, dx.at[h, RIGHT, k, dlo], fin.at[h, 0, dlo], right))
        rs(h, OPP_LEFT, ring.at[h, 1], ring.at[h, 1], partner).wait_recv()
        dx[h, LEFT, k, dhi] = dx[h, LEFT, k, dhi] + ring[h, 1]
        go(rs(h, LEFT_HI, dx.at[h, LEFT, k, dhi], fin.at[h, 1, dhi], left))

    def finish(h):
        for i, n, part in ((RIGHT_HI, 0, dhi), (RIGHT_LO, 0, dlo), (LEFT_LO, 1, dlo), (LEFT_HI, 1, dhi)):
            rs(h, i, fin.at[h, n, part], fin.at[h, n, part], partner).wait_recv()
        dn = (dx[h, OWN, k] + fin[h, 0] + fin[h, 1]).T
        xh, rstd = norm(hid[h * HT : (h + 1) * HT, :].astype(jnp.float32))
        dxh = dn * gain[...]
        m1 = jnp.mean(dxh, axis=-1, keepdims=True)
        m2 = jnp.mean(dxh * xh, axis=-1, keepdims=True)
        dh_out[h * HT : (h + 1) * HT, :] = (rstd * (dxh - m1 - xh * m2)).astype(jnp.bfloat16)
        return jnp.sum(dn * xh, axis=0, keepdims=True), jnp.sum(dn, axis=0, keepdims=True)

    def out_copy(i, slot):
        return pltpu.make_async_copy(
            stage.at[slot], de_hbm.at[pl.ds(pl.multiple_of(i * ec, ec), ec)], out_sem.at[slot]
        )

    def embed(first, last):
        @pl.loop(first, last)
        def _(i):
            slot = i % 2

            @pl.when(i >= 2)
            def _():
                out_copy(i - 2, slot).wait()

            rows = pl.ds(pl.multiple_of(i * ec, ec), ec)
            acc = None
            for tile in range(2 * CHIPS):
                xx = x_all[tile // CHIPS, tile % CHIPS].reshape(2 * HT, dim)
                part = jnp.dot(dz[tile, rows, :], xx, preferred_element_type=jnp.float32)
                acc = part if acc is None else acc + part
            stage[slot] = acc
            out_copy(i, slot).start()

    jp = 6 - 6 * k
    ref0 = tm_all.at[0]
    remote(ref0, ref0, tm_s.at[jp], tm_r.at[jp], partner).wait_recv()
    ag_arrival(0, TO_PARTNER)
    forward(0, OWN, 0)
    ag_arrival(1, TO_PARTNER)
    forward(1, OWN, 1)
    for i in range(1, group - 1):
        n = (jp + i) % (group - 1)
        remote(ref0, ref0, tm_s.at[n], tm_r.at[n], partner).wait_recv()

    def ag_pass(h):
        ag_arrival(h, TO_RIGHT)
        ag_arrival(h, TO_LEFT)
        for i in (FWD_RIGHT, FWD_LEFT, REL_RIGHT, REL_LEFT):
            go(ag_copy(h, i))

    def ag_pass_opp(h):
        ag_arrival(h, FWD_RIGHT)
        ag_arrival(h, FWD_LEFT)
        for i in (REL_OPP_A, REL_OPP_B):
            go(ag_copy(h, i))

    ag_pass(0)
    ag_arrival(0, REL_RIGHT)
    forward(0, RIGHT, 2)
    ag_pass(1)
    ag_arrival(0, REL_LEFT)
    forward(0, LEFT, 3)
    ag_pass_opp(0)
    ag_arrival(0, REL_OPP_A)
    ag_arrival(0, REL_OPP_B)
    forward(0, OPP, 4)
    stats_start(0)

    @pl.loop(0, nv)
    def _(i):
        et[i] = e[pl.ds(pl.multiple_of(i * vc, vc), vc), :].T

    ag_pass_opp(1)
    stats_finish(0)
    backward(0, OPP, 4)
    pair_start(0, OPP)
    ag_arrival(1, REL_RIGHT)
    forward(1, RIGHT, 4)
    opp_send(0)
    backward(0, RIGHT, 2)
    pair_start(0, RIGHT)
    ag_arrival(1, REL_LEFT)
    forward(1, LEFT, 2)
    right_send(0)
    backward(0, LEFT, 3)
    pair_start(0, LEFT)
    ag_arrival(1, REL_OPP_A)
    ag_arrival(1, REL_OPP_B)
    forward(1, OPP, 3)
    stats_start(1)
    left_send(0)
    ring_send(0)
    backward(0, OWN, 0)
    pair_start(0, OWN)
    stats_finish(1)
    loss_out[...] = jnp.concatenate([ls[h, pl.ds(me, 1), :] for h in range(2)], axis=0)
    both = ls[0] + ls[1]
    mean_out[...] = jnp.sum(jnp.sum(both, axis=1, keepdims=True), axis=0, keepdims=True) / token_count()
    backward(1, OPP, 3)
    pair_start(1, OPP)
    pair_finish(0, OWN)
    backward(1, RIGHT, 4)
    pair_start(1, RIGHT)
    opp_send(1)
    backward(1, LEFT, 2)
    pair_start(1, LEFT)
    right_send(1)
    backward(1, OWN, 1)
    pair_start(1, OWN)
    left_send(1)
    quarter = ne // 4
    embed(0, quarter)
    pair_finish(1, OWN)
    embed(quarter, 2 * quarter)
    ring_send(1)
    embed(2 * quarter, 3 * quarter)
    g0, b0 = finish(0)
    embed(3 * quarter, ne)
    g1, b1 = finish(1)
    g, b = g0 + g1, b0 + b1
    for i in range(4):
        gb_send[i : i + 1, :] = g[:, i * 128 : (i + 1) * 128]
        gb_send[4 + i : 5 + i, :] = b[:, i * 128 : (i + 1) * 128]

    def gb_copy(j):
        return remote(gb_send, gb_recv.at[j - 1], gb_s.at[j - 1], gb_r.at[j - 1], (me + j) % group)

    for j in range(1, group):
        go(gb_copy(j))
    for i in range(ne - 2, ne):
        out_copy(i, i % 2).wait()
    tot = gb_send[...]
    for j in range(1, group):
        gb_copy(j).wait_recv()
        tot = tot + gb_recv[j - 1]
    gb_out[...] = tot
    for copy in started:
        copy.wait_send()


def solution(mesh):
    assert mesh.shape["tp"] == 2 * CHIPS

    def group_step(hidden, ln_gain, ln_bias, out_embed, vocab_valid, targets, loss_mask):
        rows, dim = hidden.shape
        vocab = out_embed.shape[0]
        group = 2 * CHIPS
        assert rows == 2 * HT
        vc, ec = 1024, 512
        nv = vocab // vc
        f32, bf16, i32 = jnp.float32, jnp.bfloat16, jnp.int32
        vmem = pl.BlockSpec(memory_space=pltpu.VMEM)
        hbm = pl.BlockSpec(memory_space=pl.ANY)
        dma = pltpu.SemaphoreType.DMA
        loss, mean, dh, de, gb = pl.pallas_call(
            functools.partial(kernel, vc=vc, ec=ec),
            out_shape=(
                jax.ShapeDtypeStruct((2, 128), f32),
                jax.ShapeDtypeStruct((1, 1), f32),
                jax.ShapeDtypeStruct((rows, dim), bf16),
                jax.ShapeDtypeStruct((vocab, dim), f32),
                jax.ShapeDtypeStruct((8, 128), f32),
            ),
            in_specs=[vmem, vmem, vmem, hbm, vmem, vmem, vmem],
            out_specs=(vmem, vmem, vmem, hbm, vmem),
            scratch_shapes=[
                pltpu.VMEM((2, CHIPS, 2, HT, dim), bf16),
                pltpu.VMEM((dim, 2 * HT), bf16),
                pltpu.VMEM((vocab, dim), bf16),
                pltpu.VMEM((nv, dim, vc), bf16),
                pltpu.VMEM((vocab, 128), f32),
                pltpu.VMEM((5, vocab, 2 * HT), f32),
                pltpu.VMEM((2 * CHIPS, vocab, 2 * HT), bf16),
                pltpu.VMEM((group, 2, 128), i32),
                pltpu.VMEM((2, 2 * group, 128), f32),
                pltpu.VMEM((2, group - 1, 2 * group, 128), f32),
                pltpu.VMEM((2, group, 128), f32),
                pltpu.VMEM((2, group, 128), f32),
                pltpu.VMEM((2, group, 128), f32),
                pltpu.VMEM((2, CHIPS, 2, dim, HT), f32),
                pltpu.VMEM((2, CHIPS, dim, HT), f32),
                pltpu.VMEM((2, 2, dim // 2, HT), f32),
                pltpu.VMEM((2, 2, dim, HT), f32),
                pltpu.VMEM((8, 128), f32),
                pltpu.VMEM((group - 1, 8, 128), f32),
                pltpu.VMEM((2, ec, dim), f32),
                dma((nv,)),
                dma((2,)),
                dma((group - 1,)),
                dma((group - 1,)),
                dma((18,)),
                dma((18,)),
                dma((2 * (group - 1),)),
                dma((2 * (group - 1),)),
                dma((20,)),
                dma((20,)),
                dma((group - 1,)),
                dma((group - 1,)),
            ],
            compiler_params=pltpu.CompilerParams(
                collective_id=0, has_side_effects=True, vmem_limit_bytes=67043328
            ),
            name="vocab_xent",
        )(
            hidden,
            ln_gain.reshape(1, dim),
            ln_bias.reshape(1, dim),
            out_embed,
            vocab_valid.reshape(vocab // 128, 128),
            targets.reshape(2, 128),
            loss_mask.reshape(2, 128),
        )
        return (
            loss.reshape(rows),
            mean.reshape(1),
            dh,
            de,
            gb[:4].reshape(dim),
            gb[4:].reshape(dim),
        )

    row_spec = P(("dp", "tp"))
    mat_spec = P(("dp", "tp"), None)
    return jax.shard_map(
        group_step,
        mesh=mesh,
        in_specs=(mat_spec, P(None), P(None), P("tp", None), P("tp"), row_spec, row_spec),
        out_specs=(row_spec, P("dp"), mat_spec, mat_spec, P("dp"), P("dp")),
        check_vma=False,
    )
```

```python
import functools

import jax
import jax.numpy as jnp
from jax import lax
from jax.experimental import pallas as pl
from jax.experimental.pallas import tpu as pltpu
from jax.sharding import PartitionSpec as P

SOFT_CAP = 30.0
Z_COEF = 1e-4
LN_EPS = 1e-5
EXP_SCALE = SOFT_CAP * 1.4426950408889634
MESH = pl.DeviceIdType.MESH
CHIPS = 4
OFFSET = (0, 1, 3, 2)
OWN, RIGHT, LEFT, OPP = range(4)
HT = 128
CFG = (1024, 512, 1, 1, 6, 8)
SLOTS = 6
LIM = 54
SUB = 32

TO_PARTNER, TO_RIGHT, TO_LEFT, FWD_RIGHT, FWD_LEFT, REL_LEFT, REL_RIGHT, REL_OPP_A, REL_OPP_B = range(9)
PAIR, OPP_RIGHT, OPP_LEFT, RIGHT_HI, RIGHT_LO, LEFT_LO, LEFT_HI = 0, 4, 5, 6, 7, 8, 9


def norm(h):
    mean = jnp.mean(h, axis=-1, keepdims=True)
    cent = h - mean
    rstd = lax.rsqrt(jnp.mean(cent * cent, axis=-1, keepdims=True) + LN_EPS)
    return cent * rstd, rstd


def kernel(
    hid, gain, bias, e_hbm, valid, tgt, msk,
    de, loss_out, mean_out, dh_out, gain_out, bias_out,
    dz, x_all, w, xt, e, et, vb, tm_all, st_send, st_recv, av, dv, ls, dx, d2d, ring, fin, gb_send, gb_recv, iota,
    e_sem, tm_s, tm_r, ag_s, ag_r, st_s, st_r, rs_s, rs_r, gb_s, gb_r,
    *, vc, ec, fu, bu, n1, n2,
):
    group = 2 * CHIPS
    me = lax.axis_index("tp")
    c, k = me // 2, me % 2
    other = 1 - k
    partner = 2 * c + other
    chip = [(c + o) % CHIPS for o in OFFSET]
    right, left = 2 * chip[RIGHT] + k, 2 * chip[LEFT] + k
    vocab, dim = e_hbm.shape
    nv = vocab // vc

    def remote(src, dst, send, recv, dev):
        return pltpu.make_async_remote_copy(
            src_ref=src, dst_ref=dst, send_sem=send, recv_sem=recv, device_id={"tp": dev}, device_id_type=MESH
        )

    e_copies = [
        pltpu.make_async_copy(e_hbm.at[pl.ds(i * vc, vc)], e.at[pl.ds(i * vc, vc)], e_sem.at[i]) for i in range(nv)
    ]
    for cp in e_copies:
        cp.start()

    barrier = pltpu.get_barrier_semaphore()
    for j in range(1, group):
        pl.semaphore_signal(barrier, inc=1, device_id={"tp": (me + j) % group}, device_id_type=MESH)

    for h in range(2):
        xh, _ = norm(hid[h * HT : (h + 1) * HT, :].astype(jnp.float32))
        x_all[h, c, k] = (xh * gain[...] + bias[...]).astype(jnp.bfloat16)
    tm_all[me] = tgt[...] * 2 + msk[...]

    pl.semaphore_wait(barrier, group - 1)

    def ag(h, i, src, dst, dev):
        return remote(src, dst, ag_s.at[h * 9 + i], ag_r.at[h * 9 + i], dev)

    def lo(ref):
        return ref.at[pl.ds(0, HT // 2)]

    def hi(ref):
        return ref.at[pl.ds(HT // 2, HT // 2)]

    def block(h, r, core):
        return x_all.at[h, chip[r], core]

    def ag_copy(h, i):
        mine, lft, rgt, opp = block(h, OWN, k), block(h, LEFT, k), block(h, RIGHT, k), block(h, OPP, k)
        src, dev = {
            TO_PARTNER: (mine, partner),
            TO_RIGHT: (mine, right),
            TO_LEFT: (mine, left),
            FWD_RIGHT: (lo(lft), right),
            FWD_LEFT: (hi(rgt), left),
            REL_LEFT: (lft, partner),
            REL_RIGHT: (rgt, partner),
            REL_OPP_A: (lo(opp), partner),
            REL_OPP_B: (hi(opp), partner),
        }[i]
        return ag(h, i, src, src, dev)

    def ag_arrival(h, i):
        ref = {
            TO_PARTNER: block(h, OWN, other),
            TO_RIGHT: block(h, LEFT, k),
            TO_LEFT: block(h, RIGHT, k),
            FWD_RIGHT: lo(block(h, OPP, k)),
            FWD_LEFT: hi(block(h, OPP, k)),
            REL_LEFT: block(h, LEFT, other),
            REL_RIGHT: block(h, RIGHT, other),
            REL_OPP_A: lo(block(h, OPP, other)),
            REL_OPP_B: hi(block(h, OPP, other)),
        }[i]
        ag(h, i, ref, ref, partner).wait_recv()

    started = []

    def go(copy):
        copy.start()
        started.append(copy)

    def tm_copy(j):
        return remote(tm_all.at[me], tm_all.at[me], tm_s.at[j - 1], tm_r.at[j - 1], (me + j) % group)

    for h in range(2):
        if h == 0:
            for j in range(1, group):
                go(tm_copy(j))
        for i in (TO_PARTNER, TO_RIGHT, TO_LEFT) if h == 0 else (TO_PARTNER,):
            go(ag_copy(h, i))

    def tm_arrival(j):
        ref = tm_all.at[(me - j + group) % group]
        remote(ref, ref, tm_s.at[j - 1], tm_r.at[j - 1], partner).wait_recv()

    @pl.loop(0, vocab // 128)
    def _(i):
        row = jnp.broadcast_to(valid[pl.ds(i, 1), :].astype(jnp.float32), (128, 128))
        vb[pl.ds(pl.multiple_of(i * 128, 128), 128), :] = row.T

    for cp in e_copies:
        cp.wait()

    iota[...] = lax.broadcasted_iota(jnp.int32, (SUB, 128), 0)

    def local_target(h, chip_no):
        halves = [
            jnp.broadcast_to((tm_all[2 * chip_no + kk, pl.ds(h, 1), :] >> 1) - me * vocab, (8, 128)) for kk in range(2)
        ]
        return jnp.concatenate(halves, axis=1)

    def weights(slot):
        return de.at[slot] if slot < 2 else w.at[slot - 2]

    def fwd_chunk(rows0, tgt8, slot, s_acc, t_acc):
        z = jnp.dot(e[pl.ds(rows0, vc), :], xt[...], preferred_element_type=jnp.float32)
        w_c, vb_c = weights(slot).at[pl.ds(rows0, vc)], vb.at[pl.ds(rows0, vc)]
        for j in range(vc // SUB):
            rows = slice(j * SUB, j * SUB + SUB)
            ok, num = vb_c[rows, :], iota[...]
            hit = jnp.concatenate([num, num], axis=1).reshape(SUB // 8, 8, 256) == (tgt8 - (rows0 + j * SUB))[None]
            t = jnp.tanh(z[rows, :] * (1.0 / SOFT_CAP))
            ex = jnp.exp2(t * EXP_SCALE) * jnp.concatenate([ok, ok], axis=1)
            w_c[rows, :] = ex * (1.0 - t * t)
            s_acc = s_acc + jnp.sum(ex.reshape(SUB // 8, 8, 256), axis=0)
            t_acc = jnp.where(hit, t.reshape(SUB // 8, 8, 256), t_acc)
        return s_acc, t_acc

    def fwd_begin(h, r):
        xt[...] = x_all[h, chip[r]].reshape(2 * HT, dim).T
        return local_target(h, chip[r])

    def fwd_end(h, r, s_acc, t_acc):
        s_row = jnp.sum(s_acc, axis=0, keepdims=True)
        t_row = jnp.sum(t_acc.reshape(SUB, 256), axis=0, keepdims=True)
        for kk in range(2):
            st_send[h, pl.ds(2 * chip[r] + kk, 1), :] = s_row[:, kk * 128 : (kk + 1) * 128]
            st_send[h, pl.ds(group + 2 * chip[r] + kk, 1), :] = t_row[:, kk * 128 : (kk + 1) * 128]

    zero = (jnp.zeros((8, 256), jnp.float32), jnp.zeros((SUB // 8, 8, 256), jnp.float32))

    def forward(h, r, slot):
        tgt8 = fwd_begin(h, r)

        def body(i, carry):
            for u in range(fu):
                carry = fwd_chunk(pl.multiple_of((i * fu + u) * vc, vc), tgt8, slot, *carry)
            return carry

        fwd_end(h, r, *lax.fori_loop(0, nv // fu, body, zero))

    def st_copy(h, j):
        n = h * (group - 1) + j - 1
        return remote(st_send.at[h], st_recv.at[h, j - 1], st_s.at[n], st_r.at[n], (me + j) % group)

    def stats_start(h):
        for j in range(1, group):
            go(st_copy(h, j))

    def token_count():
        total = jnp.zeros((2, 128), jnp.int32)
        for p in range(group):
            total = total + (tm_all[p] & 1)
        total = jnp.sum(jnp.sum(total.astype(jnp.float32), axis=1, keepdims=True), axis=0, keepdims=True)
        return total

    def stats_finish(h):
        tot = st_send[h]
        for j in range(1, group):
            st_copy(h, j).wait_recv()
        for j in range(1, group):
            tot = tot + st_recv[h, j - 1]
        s, t = tot[:group], tot[group:]
        mask = jnp.concatenate([tm_all[p, pl.ds(h, 1), :] & 1 for p in range(group)], axis=0).astype(jnp.float32)
        lse = jnp.log(s)
        coef = mask / token_count()
        a = (1.0 + 2.0 * Z_COEF * lse) * coef / s
        av[h] = a
        dv[h] = (a * jnp.exp2(t * EXP_SCALE) - coef) * (1.0 - t * t)
        ls[h] = (lse - SOFT_CAP * t + Z_COEF * lse * lse) * mask

    def spread(ref, h, chip_no):
        return jnp.concatenate(
            [jnp.broadcast_to(ref[h, pl.ds(2 * chip_no + kk, 1), :], (8, 128)) for kk in range(2)], axis=1
        )

    def bwd_begin(h, r):
        for kk in range(2):
            dx[h, r, kk] = jnp.zeros((dim, HT), jnp.float32)
        return local_target(h, chip[r]), spread(av, h, chip[r]), spread(dv, h, chip[r])

    def bwd_chunk(i, h, r, slot, tgt8, a8, d8):
        rows0 = pl.multiple_of(i * vc, vc)
        pieces = []
        w_c, dz_c = weights(slot).at[pl.ds(rows0, vc)], dz.at[h * CHIPS + chip[r], pl.ds(rows0, vc)]
        for j in range(vc // SUB):
            rows = slice(j * SUB, j * SUB + SUB)
            num = iota[...]
            hit = jnp.concatenate([num, num], axis=1).reshape(SUB // 8, 8, 256) == (tgt8 - (rows0 + j * SUB))[None]
            g = jnp.where(hit, d8[None], a8[None] * w_c[rows, :].reshape(SUB // 8, 8, 256))
            g = g.reshape(SUB, 256).astype(jnp.bfloat16)
            dz_c[rows, :] = g
            pieces.append(g)
        return jnp.dot(et[i], jnp.concatenate(pieces, axis=0), preferred_element_type=jnp.float32)

    def bwd_add(h, r, part):
        for kk in range(2):
            dx[h, r, kk] += part[:, kk * HT : (kk + 1) * HT]

    def backward(h, r, slot):
        vecs = bwd_begin(h, r)

        @pl.loop(0, nv // bu)
        def _(i):
            part = None
            for u in range(bu):
                more = bwd_chunk(i * bu + u, h, r, slot, *vecs)
                part = more if part is None else part + more
            bwd_add(h, r, part)

    def both(hb, rb, hf, rf, slot):
        vecs = bwd_begin(hb, rb)
        tgt8 = fwd_begin(hf, rf)

        def body(i, carry):
            part = bwd_chunk(i, hb, rb, slot, *vecs)
            carry = fwd_chunk(pl.multiple_of(i * vc, vc), tgt8, slot, *carry)
            bwd_add(hb, rb, part)
            return carry

        fwd_end(hf, rf, *lax.fori_loop(0, nv, body, zero))

    dlo, dhi = pl.ds(0, dim // 2), pl.ds(dim // 2, dim // 2)

    def rs(h, i, src, dst, dev):
        return remote(src, dst, rs_s.at[h * 10 + i], rs_r.at[h * 10 + i], dev)

    def pair_start(h, r):
        go(rs(h, PAIR + r, dx.at[h, r, other], d2d.at[h, r], partner))

    def pair_finish(h, r):
        rs(h, PAIR + r, d2d.at[h, r], d2d.at[h, r], partner).wait_recv()
        dx[h, r, k] = dx[h, r, k] + d2d[h, r]

    def opp_send(h):
        pair_finish(h, OPP)
        go(rs(h, OPP_RIGHT, dx.at[h, OPP, k, dlo], ring.at[h, 0], right))
        go(rs(h, OPP_LEFT, dx.at[h, OPP, k, dhi], ring.at[h, 1], left))

    def right_send(h):
        pair_finish(h, RIGHT)
        go(rs(h, RIGHT_HI, dx.at[h, RIGHT, k, dhi], fin.at[h, 0, dhi], right))

    def left_send(h):
        pair_finish(h, LEFT)
        go(rs(h, LEFT_LO, dx.at[h, LEFT, k, dlo], fin.at[h, 1, dlo], left))

    def ring_send(h):
        rs(h, OPP_RIGHT, ring.at[h, 0], ring.at[h, 0], partner).wait_recv()
        dx[h, RIGHT, k, dlo] = dx[h, RIGHT, k, dlo] + ring[h, 0]
        go(rs(h, RIGHT_LO, dx.at[h, RIGHT, k, dlo], fin.at[h, 0, dlo], right))
        rs(h, OPP_LEFT, ring.at[h, 1], ring.at[h, 1], partner).wait_recv()
        dx[h, LEFT, k, dhi] = dx[h, LEFT, k, dhi] + ring[h, 1]
        go(rs(h, LEFT_HI, dx.at[h, LEFT, k, dhi], fin.at[h, 1, dhi], left))

    def finish(h):
        for i, n, part in ((RIGHT_HI, 0, dhi), (RIGHT_LO, 0, dlo), (LEFT_LO, 1, dlo), (LEFT_HI, 1, dhi)):
            rs(h, i, fin.at[h, n, part], fin.at[h, n, part], partner).wait_recv()
        dn = (dx[h, OWN, k] + fin[h, 0] + fin[h, 1]).T
        xh, rstd = norm(hid[h * HT : (h + 1) * HT, :].astype(jnp.float32))
        dxh = dn * gain[...]
        m1 = jnp.mean(dxh, axis=-1, keepdims=True)
        m2 = jnp.mean(dxh * xh, axis=-1, keepdims=True)
        dh_out[h * HT : (h + 1) * HT, :] = (rstd * (dxh - m1 - xh * m2)).astype(jnp.bfloat16)
        return jnp.sum(dn * xh, axis=0, keepdims=True), jnp.sum(dn, axis=0, keepdims=True)

    def embed(first, last):
        @pl.loop(first, last)
        def _(i):
            rows = pl.ds(pl.multiple_of(i * ec, ec), ec)
            acc = embed_rows(dz, x_all, rows)
            for half in range(2):
                de[half, rows, :] = acc[:, half * 256 : (half + 1) * 256]

    jp = 6 - 6 * k
    ref0 = tm_all.at[0]

    def ag_pass(h):
        ag_arrival(h, TO_RIGHT)
        ag_arrival(h, TO_LEFT)
        for i in (FWD_RIGHT, FWD_LEFT, REL_RIGHT, REL_LEFT):
            go(ag_copy(h, i))

    def ag_pass_opp(h):
        ag_arrival(h, FWD_RIGHT)
        ag_arrival(h, FWD_LEFT)
        for i in (REL_OPP_A, REL_OPP_B):
            go(ag_copy(h, i))

    remote(ref0, ref0, tm_s.at[jp], tm_r.at[jp], partner).wait_recv()
    ag_arrival(0, TO_PARTNER)
    forward(0, OWN, 0)
    ag_arrival(1, TO_PARTNER)
    forward(1, OWN, 1)
    for i in range(1, group - 1):
        n = (jp + i) % (group - 1)
        remote(ref0, ref0, tm_s.at[n], tm_r.at[n], partner).wait_recv()
    ag_pass(0)
    go(ag_copy(1, TO_RIGHT))
    go(ag_copy(1, TO_LEFT))

    @pl.loop(0, nv)
    def _(i):
        et[i] = e[pl.ds(pl.multiple_of(i * vc, vc), vc), :].T

    ag_arrival(0, REL_RIGHT)
    forward(0, RIGHT, 2)
    ag_pass_opp(0)
    ag_arrival(0, REL_LEFT)
    forward(0, LEFT, 3)
    ag_pass(1)
    ag_arrival(0, REL_OPP_A)
    ag_arrival(0, REL_OPP_B)
    forward(0, OPP, 4)
    stats_start(0)
    ag_arrival(1, REL_RIGHT)
    forward(1, RIGHT, 5)
    ag_pass_opp(1)
    stats_finish(0)
    ag_arrival(1, REL_LEFT)
    both(0, OPP, 1, LEFT, 4)
    pair_start(0, OPP)
    ag_arrival(1, REL_OPP_A)
    ag_arrival(1, REL_OPP_B)
    both(0, RIGHT, 1, OPP, 2)
    stats_start(1)
    pair_start(0, RIGHT)
    opp_send(0)
    backward(0, LEFT, 3)
    pair_start(0, LEFT)
    right_send(0)
    backward(0, OWN, 0)
    pair_start(0, OWN)
    left_send(0)
    stats_finish(1)
    loss_out[...] = jnp.concatenate([ls[h, pl.ds(me, 1), :] for h in range(2)], axis=0)
    total = ls[0] + ls[1]
    mean_out[...] = jnp.sum(jnp.sum(total, axis=1, keepdims=True), axis=0, keepdims=True) / token_count()
    backward(1, OPP, 2)
    pair_start(1, OPP)
    ring_send(0)
    backward(1, RIGHT, 5)
    pair_start(1, RIGHT)
    opp_send(1)
    backward(1, LEFT, 4)
    pair_start(1, LEFT)
    right_send(1)
    backward(1, OWN, 1)
    pair_start(1, OWN)
    left_send(1)
    embed(0, 2)
    ring_send(1)
    pair_finish(0, OWN)
    pair_finish(1, OWN)
    g0, b0 = finish(0)
    embed(2, n1)
    g1, b1 = finish(1)
    g, b = g0 + g1, b0 + b1
    for i in range(4):
        gb_send[i : i + 1, :] = g[:, i * 128 : (i + 1) * 128]
        gb_send[4 + i : 5 + i, :] = b[:, i * 128 : (i + 1) * 128]

    def gb_copy(j):
        return remote(gb_send, gb_recv.at[j - 1], gb_s.at[j - 1], gb_r.at[j - 1], (me + j) % group)

    for j in range(1, group):
        go(gb_copy(j))
    embed(n1, n2)
    tot = gb_send[...]
    for j in range(1, group):
        gb_copy(j).wait_recv()
        tot = tot + gb_recv[j - 1]
    gain_out[...], bias_out[...] = tot[:4], tot[4:]
    for copy in started:
        copy.wait_send()


def embed_rows(dz, x_all, rows):
    acc = None
    for tile in range(2 * CHIPS):
        xx = x_all[tile // CHIPS, tile % CHIPS].reshape(2 * HT, -1)
        part = jnp.dot(dz[tile, rows, :], xx, preferred_element_type=jnp.float32)
        acc = part if acc is None else acc + part
    return acc


def write_out(
    de, loss_in, mean_in, dh_in, gain_in, bias_in,
    loss_out, mean_out, dh_out, de_hbm, gain_out, bias_out,
    sems, *, pieces,
):
    rows = de_hbm.shape[0] // pieces
    half = de_hbm.shape[1] // 2
    copies = []

    def go(src, dst):
        copies.append(pltpu.make_async_copy(src, dst, sems.at[len(copies)]))
        copies[-1].start()

    for i in range(pieces):
        part = pl.ds(i * rows, rows)
        for c in range(2):
            go(de.at[c, part], de_hbm.at[part, pl.ds(c * half, half)])
    for src, dst in ((dh_in, dh_out), (loss_in, loss_out), (gain_in, gain_out), (bias_in, bias_out)):
        go(src, dst)
    mean_out[...] = mean_in[...]
    for copy in copies:
        copy.wait()


def solution(mesh):
    assert mesh.shape["tp"] == 2 * CHIPS

    def group_step(hidden, ln_gain, ln_bias, out_embed, vocab_valid, targets, loss_mask):
        rows, dim = hidden.shape
        vocab = out_embed.shape[0]
        group = 2 * CHIPS
        assert rows == 2 * HT
        vc, ec, fu, bu, n1, n2 = CFG
        nv = vocab // vc
        f32, bf16, i32 = jnp.float32, jnp.bfloat16, jnp.int32
        vmem = pl.BlockSpec(memory_space=pltpu.VMEM)
        hbm = pl.BlockSpec(memory_space=pl.ANY)
        dma = pltpu.SemaphoreType.DMA
        results = pl.pallas_call(
            functools.partial(kernel, vc=vc, ec=ec, fu=fu, bu=bu, n1=n1, n2=n2),
            out_shape=(
                pltpu.VMEM((2, vocab, dim // 2), f32),
                pltpu.VMEM((2, 128), f32),
                pltpu.VMEM((1, 1), f32),
                pltpu.VMEM((rows, dim), bf16),
                pltpu.VMEM((4, 128), f32),
                pltpu.VMEM((4, 128), f32),
            ),
            in_specs=[vmem, vmem, vmem, hbm, vmem, vmem, vmem],
            out_specs=(vmem,) * 6,
            scratch_shapes=[
                pltpu.VMEM((2 * CHIPS, vocab, 2 * HT), bf16),
                pltpu.VMEM((2, CHIPS, 2, HT, dim), bf16),
                pltpu.VMEM((SLOTS - 2, vocab, 2 * HT), f32),
                pltpu.VMEM((dim, 2 * HT), bf16),
                pltpu.VMEM((vocab, dim), bf16),
                pltpu.VMEM((nv, dim, vc), bf16),
                pltpu.VMEM((vocab, 128), f32),
                pltpu.VMEM((group, 2, 128), i32),
                pltpu.VMEM((2, 2 * group, 128), f32),
                pltpu.VMEM((2, group - 1, 2 * group, 128), f32),
                pltpu.VMEM((2, group, 128), f32),
                pltpu.VMEM((2, group, 128), f32),
                pltpu.VMEM((2, group, 128), f32),
                pltpu.VMEM((2, CHIPS, 2, dim, HT), f32),
                pltpu.VMEM((2, CHIPS, dim, HT), f32),
                pltpu.VMEM((2, 2, dim // 2, HT), f32),
                pltpu.VMEM((2, 2, dim, HT), f32),
                pltpu.VMEM((8, 128), f32),
                pltpu.VMEM((group - 1, 8, 128), f32),
                pltpu.VMEM((SUB, 128), i32),
                dma((nv,)),
                dma((group - 1,)),
                dma((group - 1,)),
                dma((18,)),
                dma((18,)),
                dma((2 * (group - 1),)),
                dma((2 * (group - 1),)),
                dma((20,)),
                dma((20,)),
                dma((group - 1,)),
                dma((group - 1,)),
            ],
            compiler_params=pltpu.CompilerParams(
                collective_id=0, has_side_effects=True, vmem_limit_bytes=LIM << 20
            ),
            name="vocab_xent",
        )(
            hidden,
            ln_gain.reshape(1, dim),
            ln_bias.reshape(1, dim),
            out_embed,
            vocab_valid.reshape(vocab // 128, 128),
            targets.reshape(2, 128),
            loss_mask.reshape(2, 128),
        )
        loss, mean, dh, de, dgain, dbias = pl.pallas_call(
            functools.partial(write_out, pieces=4),
            out_shape=(
                jax.ShapeDtypeStruct((2, 128), f32),
                jax.ShapeDtypeStruct((1, 1), f32),
                jax.ShapeDtypeStruct((rows, dim), bf16),
                jax.ShapeDtypeStruct((vocab, dim), f32),
                jax.ShapeDtypeStruct((4, 128), f32),
                jax.ShapeDtypeStruct((4, 128), f32),
            ),
            in_specs=[vmem] * 6,
            out_specs=(hbm, vmem, hbm, hbm, hbm, hbm),
            scratch_shapes=[dma((12,))],
            compiler_params=pltpu.CompilerParams(vmem_limit_bytes=2 << 20),
            name="write_out",
        )(*results)
        return (
            loss.reshape(rows),
            mean.reshape(1),
            dh,
            de,
            dgain.reshape(dim),
            dbias.reshape(dim),
        )

    row_spec = P(("dp", "tp"))
    mat_spec = P(("dp", "tp"), None)
    return jax.shard_map(
        group_step,
        mesh=mesh,
        in_specs=(mat_spec, P(None), P(None), P("tp", None), P("tp"), row_spec, row_spec),
        out_specs=(row_spec, P("dp"), mat_spec, mat_spec, P("dp"), P("dp")),
        check_vma=False,
    )
```

```python
import functools

import jax
import jax.numpy as jnp
from jax import lax
from jax.experimental import pallas as pl
from jax.experimental.pallas import tpu as pltpu
from jax.sharding import PartitionSpec as P

SOFT_CAP = 30.0
Z_COEF = 1e-4
LN_EPS = 1e-5
EXP_SCALE = SOFT_CAP * 1.4426950408889634
MESH = pl.DeviceIdType.MESH
CHIPS = 4
OFFSET = (0, 1, 3, 2)
OWN, RIGHT, LEFT, OPP = range(4)
GRADS = ((0, OPP), (0, RIGHT), (0, LEFT), (0, OWN), (1, OPP), (1, RIGHT), (1, LEFT), (1, OWN))
HT = 128
CFG = (512, 512, 6, 8)
FS, BS, CS = 2048, 2048, 1024
SLOTS = 6
LIM = 54 * 2**20
SUB = 32

TO_PARTNER, TO_RIGHT, TO_LEFT, FWD_RIGHT, FWD_LEFT, REL_LEFT, REL_RIGHT, REL_OPP_A, REL_OPP_B = range(9)
PAIR, OPP_RIGHT, OPP_LEFT, RIGHT_HI, RIGHT_LO, LEFT_LO, LEFT_HI = 0, 4, 5, 6, 7, 8, 9


def norm(h):
    mean = jnp.mean(h, axis=-1, keepdims=True)
    cent = h - mean
    rstd = lax.rsqrt(jnp.mean(cent * cent, axis=-1, keepdims=True) + LN_EPS)
    return cent * rstd, rstd


def kernel(
    hid, gain, bias, e_hbm, valid, tgt, msk,
    de, loss_out, mean_out, dh_out, gain_out, bias_out,
    dz, x_all, w, xt, e, et, vb, tm_all, st_send, st_recv, av, dv, ls, dx, d2d, ring, fin, gb_send, gb_recv, iota,
    e_sem, tm_s, tm_r, ag_s, ag_r, st_s, st_r, rs_s, rs_r, gb_s, gb_r,
    *, vc, ec, n1, n2,
):
    group = 2 * CHIPS
    me = lax.axis_index("tp")
    c, k = me // 2, me % 2
    other = 1 - k
    partner = 2 * c + other
    chip = [(c + o) % CHIPS for o in OFFSET]
    right, left = 2 * chip[RIGHT] + k, 2 * chip[LEFT] + k
    vocab, dim = e_hbm.shape
    nv = vocab // vc

    def remote(src, dst, send, recv, dev):
        return pltpu.make_async_remote_copy(
            src_ref=src, dst_ref=dst, send_sem=send, recv_sem=recv, device_id={"tp": dev}, device_id_type=MESH
        )

    e_copies = [
        pltpu.make_async_copy(e_hbm.at[pl.ds(i * vc, vc)], e.at[pl.ds(i * vc, vc)], e_sem.at[i]) for i in range(nv)
    ]
    for cp in e_copies:
        cp.start()

    barrier = pltpu.get_barrier_semaphore()
    for j in range(1, group):
        pl.semaphore_signal(barrier, inc=1, device_id={"tp": (me + j) % group}, device_id_type=MESH)

    for h in range(2):
        xh, _ = norm(hid[h * HT : (h + 1) * HT, :].astype(jnp.float32))
        x_all[h, c, k] = (xh * gain[...] + bias[...]).astype(jnp.bfloat16)
    tm_all[me] = tgt[...] * 2 + msk[...]

    pl.semaphore_wait(barrier, group - 1)

    def ag(h, i, src, dst, dev):
        return remote(src, dst, ag_s.at[h * 9 + i], ag_r.at[h * 9 + i], dev)

    def lo(ref):
        return ref.at[pl.ds(0, HT // 2)]

    def hi(ref):
        return ref.at[pl.ds(HT // 2, HT // 2)]

    def block(h, r, core):
        return x_all.at[h, chip[r], core]

    def ag_copy(h, i):
        mine, lft, rgt, opp = block(h, OWN, k), block(h, LEFT, k), block(h, RIGHT, k), block(h, OPP, k)
        src, dev = {
            TO_PARTNER: (mine, partner),
            TO_RIGHT: (mine, right),
            TO_LEFT: (mine, left),
            FWD_RIGHT: (lo(lft), right),
            FWD_LEFT: (hi(rgt), left),
            REL_LEFT: (lft, partner),
            REL_RIGHT: (rgt, partner),
            REL_OPP_A: (lo(opp), partner),
            REL_OPP_B: (hi(opp), partner),
        }[i]
        return ag(h, i, src, src, dev)

    def ag_arrival(h, i):
        ref = {
            TO_PARTNER: block(h, OWN, other),
            TO_RIGHT: block(h, LEFT, k),
            TO_LEFT: block(h, RIGHT, k),
            FWD_RIGHT: lo(block(h, OPP, k)),
            FWD_LEFT: hi(block(h, OPP, k)),
            REL_LEFT: block(h, LEFT, other),
            REL_RIGHT: block(h, RIGHT, other),
            REL_OPP_A: lo(block(h, OPP, other)),
            REL_OPP_B: hi(block(h, OPP, other)),
        }[i]
        ag(h, i, ref, ref, partner).wait_recv()

    started = []

    def go(copy):
        copy.start()
        started.append(copy)

    def tm_copy(j):
        return remote(tm_all.at[me], tm_all.at[me], tm_s.at[j - 1], tm_r.at[j - 1], (me + j) % group)

    for h in range(2):
        if h == 0:
            for j in range(1, group):
                go(tm_copy(j))
        for i in (TO_PARTNER, TO_RIGHT, TO_LEFT):
            go(ag_copy(h, i))

    def tm_arrival(j):
        ref = tm_all.at[(me - j + group) % group]
        remote(ref, ref, tm_s.at[j - 1], tm_r.at[j - 1], partner).wait_recv()

    @pl.loop(0, vocab // 128)
    def _(i):
        row = jnp.broadcast_to(valid[pl.ds(i, 1), :].astype(jnp.float32), (128, 128))
        vb[pl.ds(pl.multiple_of(i * 128, 128), 128), :] = row.T

    for cp in e_copies:
        cp.wait()

    iota[...] = lax.broadcasted_iota(jnp.int32, (SUB, 128), 0)

    def local_target(h, chip_no):
        halves = [
            jnp.broadcast_to((tm_all[2 * chip_no + kk, pl.ds(h, 1), :] >> 1) - me * vocab, (8, 128)) for kk in range(2)
        ]
        return jnp.concatenate(halves, axis=1)

    def weights(slot):
        return de.at[slot] if slot < 2 else w.at[slot - 2]

    def fwd_begin(tiles):
        for n, (h, r, _) in enumerate(tiles):
            xt[:, n * 256 : (n + 1) * 256] = x_all[h, chip[r]].reshape(2 * HT, dim).T
        return [local_target(h, chip[r]) for h, r, _ in tiles]

    def softmax_part(rows0, size, tgts, tiles, carry):
        count = len(tiles)
        z = jnp.dot(e[pl.ds(rows0, size), :], xt[:, : count * 256], preferred_element_type=jnp.float32)
        vb_c = vb.at[pl.ds(rows0, size)]
        outs = [weights(slot).at[pl.ds(rows0, size)] for _, _, slot in tiles]
        carry = list(carry)
        for j in range(size // SUB):
            rows = slice(j * SUB, j * SUB + SUB)
            ok, num = vb_c[rows, :], iota[...]
            ok = jnp.concatenate([ok, ok], axis=1)
            num = jnp.concatenate([num, num], axis=1).reshape(SUB // 8, 8, 256)
            for n in range(count):
                s_acc, t_acc = carry[n]
                t = jnp.tanh(z[rows, n * 256 : (n + 1) * 256] * (1.0 / SOFT_CAP))
                ex = jnp.exp2(t * EXP_SCALE) * ok
                outs[n][rows, :] = ex * (1.0 - t * t)
                hit = num == (tgts[n] - (rows0 + j * SUB))[None]
                s_acc = s_acc + jnp.sum(ex.reshape(SUB // 8, 8, 256), axis=0)
                t_acc = jnp.where(hit, t.reshape(SUB // 8, 8, 256), t_acc)
                carry[n] = s_acc, t_acc
        return tuple(carry)

    def fwd_end(tiles, carry):
        for (h, r, _), (s_acc, t_acc) in zip(tiles, carry):
            s_row = jnp.sum(s_acc, axis=0, keepdims=True)
            t_row = jnp.sum(t_acc.reshape(SUB, 256), axis=0, keepdims=True)
            for kk in range(2):
                st_send[h, pl.ds(2 * chip[r] + kk, 1), :] = s_row[:, kk * 128 : (kk + 1) * 128]
                st_send[h, pl.ds(group + 2 * chip[r] + kk, 1), :] = t_row[:, kk * 128 : (kk + 1) * 128]

    def fwd_zero(tiles):
        zero = (jnp.zeros((8, 256), jnp.float32), jnp.zeros((SUB // 8, 8, 256), jnp.float32))
        return tuple(zero for _ in tiles)

    def forward(*tiles):
        size = FS
        steps = vocab // size
        tgts = fwd_begin(tiles)

        def body(i, carry):
            return softmax_part(pl.multiple_of(i * size, size), size, tgts, tiles, carry)

        fwd_end(tiles, lax.fori_loop(0, steps, body, fwd_zero(tiles)))

    def st_copy(h, j):
        n = h * (group - 1) + j - 1
        return remote(st_send.at[h], st_recv.at[h, j - 1], st_s.at[n], st_r.at[n], (me + j) % group)

    def stats_start(h):
        for j in range(1, group):
            go(st_copy(h, j))

    def token_count():
        total = jnp.zeros((2, 128), jnp.int32)
        for p in range(group):
            total = total + (tm_all[p] & 1)
        total = jnp.sum(jnp.sum(total.astype(jnp.float32), axis=1, keepdims=True), axis=0, keepdims=True)
        return total

    def stats_finish(h):
        tot = st_send[h]
        for j in range(1, group):
            st_copy(h, j).wait_recv()
        for j in range(1, group):
            tot = tot + st_recv[h, j - 1]
        s, t = tot[:group], tot[group:]
        mask = jnp.concatenate([tm_all[p, pl.ds(h, 1), :] & 1 for p in range(group)], axis=0).astype(jnp.float32)
        lse = jnp.log(s)
        coef = mask / token_count()
        a = (1.0 + 2.0 * Z_COEF * lse) * coef / s
        av[h] = a
        dv[h] = (a * jnp.exp2(t * EXP_SCALE) - coef) * (1.0 - t * t)
        ls[h] = (lse - SOFT_CAP * t + Z_COEF * lse * lse) * mask

    def spread(ref, h, chip_no):
        return jnp.concatenate(
            [jnp.broadcast_to(ref[h, pl.ds(2 * chip_no + kk, 1), :], (8, 128)) for kk in range(2)], axis=1
        )

    def bwd_begin(h, r):
        for kk in range(2):
            dx[h, r, kk] = jnp.zeros((dim, HT), jnp.float32)
        return local_target(h, chip[r]), spread(av, h, chip[r]), spread(dv, h, chip[r])

    def grad_store(h, r):
        n = GRADS.index((h, r))
        return dz.at[n] if n < 6 else e.at[:, pl.ds((n - 6) * 256, 256)]

    def hidden_part(i, size, h, r, slot, tgt8, a8, d8):
        rows0 = pl.multiple_of(i * size, size)
        w_c, dz_c = weights(slot).at[pl.ds(rows0, size)], grad_store(h, r).at[pl.ds(rows0, size)]
        part = None
        for u in range(size // vc):
            pieces = []
            for j in range(u * vc // SUB, (u + 1) * vc // SUB):
                rows = slice(j * SUB, j * SUB + SUB)
                num = iota[...]
                hit = jnp.concatenate([num, num], axis=1).reshape(SUB // 8, 8, 256) == (tgt8 - (rows0 + j * SUB))[None]
                g = jnp.where(hit, d8[None], a8[None] * w_c[rows, :].reshape(SUB // 8, 8, 256))
                g = g.reshape(SUB, 256).astype(jnp.bfloat16)
                dz_c[rows, :] = g
                pieces.append(g)
            more = jnp.dot(
                et[i * (size // vc) + u], jnp.concatenate(pieces, axis=0), preferred_element_type=jnp.float32
            )
            part = more if part is None else part + more
        return part

    def bwd_add(h, r, part):
        for kk in range(2):
            dx[h, r, kk] += part[:, kk * HT : (kk + 1) * HT]

    def backward(h, r, slot):
        vecs = bwd_begin(h, r)

        @pl.loop(0, vocab // BS)
        def _(i):
            bwd_add(h, r, hidden_part(i, BS, h, r, slot, *vecs))

    def both(hb, rb, hf, rf, slot):
        tile = ((hf, rf, slot),)
        vecs = bwd_begin(hb, rb)
        tgts = fwd_begin(tile)

        def body(i, carry):
            part = hidden_part(i, CS, hb, rb, slot, *vecs)
            carry = softmax_part(pl.multiple_of(i * CS, CS), CS, tgts, tile, carry)
            bwd_add(hb, rb, part)
            return carry

        fwd_end(tile, lax.fori_loop(0, vocab // CS, body, fwd_zero(tile)))

    dlo, dhi = pl.ds(0, dim // 2), pl.ds(dim // 2, dim // 2)

    def rs(h, i, src, dst, dev):
        return remote(src, dst, rs_s.at[h * 10 + i], rs_r.at[h * 10 + i], dev)

    def pair_start(h, r):
        go(rs(h, PAIR + r, dx.at[h, r, other], d2d.at[h, r], partner))

    def pair_finish(h, r):
        rs(h, PAIR + r, d2d.at[h, r], d2d.at[h, r], partner).wait_recv()
        dx[h, r, k] = dx[h, r, k] + d2d[h, r]

    def opp_send(h):
        pair_finish(h, OPP)
        go(rs(h, OPP_RIGHT, dx.at[h, OPP, k, dlo], ring.at[h, 0], right))
        go(rs(h, OPP_LEFT, dx.at[h, OPP, k, dhi], ring.at[h, 1], left))

    def right_send(h):
        pair_finish(h, RIGHT)
        go(rs(h, RIGHT_HI, dx.at[h, RIGHT, k, dhi], fin.at[h, 0, dhi], right))

    def left_send(h):
        pair_finish(h, LEFT)
        go(rs(h, LEFT_LO, dx.at[h, LEFT, k, dlo], fin.at[h, 1, dlo], left))

    def ring_send(h):
        rs(h, OPP_RIGHT, ring.at[h, 0], ring.at[h, 0], partner).wait_recv()
        dx[h, RIGHT, k, dlo] = dx[h, RIGHT, k, dlo] + ring[h, 0]
        go(rs(h, RIGHT_LO, dx.at[h, RIGHT, k, dlo], fin.at[h, 0, dlo], right))
        rs(h, OPP_LEFT, ring.at[h, 1], ring.at[h, 1], partner).wait_recv()
        dx[h, LEFT, k, dhi] = dx[h, LEFT, k, dhi] + ring[h, 1]
        go(rs(h, LEFT_HI, dx.at[h, LEFT, k, dhi], fin.at[h, 1, dhi], left))

    def finish(h):
        for i, n, part in ((RIGHT_HI, 0, dhi), (RIGHT_LO, 0, dlo), (LEFT_LO, 1, dlo), (LEFT_HI, 1, dhi)):
            rs(h, i, fin.at[h, n, part], fin.at[h, n, part], partner).wait_recv()
        dn = (dx[h, OWN, k] + fin[h, 0] + fin[h, 1]).T
        xh, rstd = norm(hid[h * HT : (h + 1) * HT, :].astype(jnp.float32))
        dxh = dn * gain[...]
        m1 = jnp.mean(dxh, axis=-1, keepdims=True)
        m2 = jnp.mean(dxh * xh, axis=-1, keepdims=True)
        dh_out[h * HT : (h + 1) * HT, :] = (rstd * (dxh - m1 - xh * m2)).astype(jnp.bfloat16)
        return jnp.sum(dn * xh, axis=0, keepdims=True), jnp.sum(dn, axis=0, keepdims=True)

    def embed_rows(rows):
        acc = None
        for h in range(2):
            for r in range(CHIPS):
                xx = x_all[h, chip[r]].reshape(2 * HT, dim)
                part = jnp.dot(grad_store(h, r)[rows, :], xx, preferred_element_type=jnp.float32)
                acc = part if acc is None else acc + part
        return acc

    def embed(first, last):
        @pl.loop(first, last)
        def _(i):
            rows = pl.ds(pl.multiple_of(i * ec, ec), ec)
            acc = embed_rows(rows)
            for half in range(2):
                de[half, rows, :] = acc[:, half * 256 : (half + 1) * 256]

    jp = 6 - 6 * k
    ref0 = tm_all.at[0]

    def ag_pass(h):
        ag_arrival(h, TO_RIGHT)
        ag_arrival(h, TO_LEFT)
        for i in (FWD_RIGHT, FWD_LEFT, REL_RIGHT, REL_LEFT):
            go(ag_copy(h, i))

    def ag_pass_opp(h):
        ag_arrival(h, FWD_RIGHT)
        ag_arrival(h, FWD_LEFT)
        for i in (REL_OPP_A, REL_OPP_B):
            go(ag_copy(h, i))

    remote(ref0, ref0, tm_s.at[jp], tm_r.at[jp], partner).wait_recv()
    ag_arrival(0, TO_PARTNER)
    ag_arrival(1, TO_PARTNER)
    forward((0, OWN, 0))
    forward((1, OWN, 1))
    for i in range(1, group - 1):
        n = (jp + i) % (group - 1)
        remote(ref0, ref0, tm_s.at[n], tm_r.at[n], partner).wait_recv()
    ag_pass(0)

    @pl.loop(0, nv)
    def _(i):
        et[i] = e[pl.ds(pl.multiple_of(i * vc, vc), vc), :].T

    ag_arrival(0, REL_RIGHT)
    forward((0, RIGHT, 2))
    ag_pass(1)
    ag_pass_opp(0)
    ag_arrival(0, REL_LEFT)
    forward((0, LEFT, 3))
    ag_arrival(0, REL_OPP_A)
    ag_arrival(0, REL_OPP_B)
    forward((0, OPP, 4))
    stats_start(0)
    ag_pass_opp(1)
    ag_arrival(1, REL_RIGHT)
    forward((1, RIGHT, 5))
    stats_finish(0)
    ag_arrival(1, REL_LEFT)
    both(0, OPP, 1, LEFT, 4)
    pair_start(0, OPP)
    ag_arrival(1, REL_OPP_A)
    ag_arrival(1, REL_OPP_B)
    both(0, RIGHT, 1, OPP, 2)
    stats_start(1)
    pair_start(0, RIGHT)
    opp_send(0)
    backward(0, LEFT, 3)
    pair_start(0, LEFT)
    right_send(0)
    backward(0, OWN, 0)
    pair_start(0, OWN)
    left_send(0)
    stats_finish(1)
    loss_out[...] = jnp.concatenate([ls[h, pl.ds(me, 1), :] for h in range(2)], axis=0)
    total = ls[0] + ls[1]
    mean_out[...] = jnp.sum(jnp.sum(total, axis=1, keepdims=True), axis=0, keepdims=True) / token_count()
    backward(1, OPP, 2)
    pair_start(1, OPP)
    ring_send(0)
    backward(1, RIGHT, 5)
    pair_start(1, RIGHT)
    opp_send(1)
    backward(1, LEFT, 4)
    pair_start(1, LEFT)
    right_send(1)
    backward(1, OWN, 1)
    pair_start(1, OWN)
    left_send(1)
    embed(0, 2)
    ring_send(1)
    pair_finish(0, OWN)
    pair_finish(1, OWN)
    g0, b0 = finish(0)
    embed(2, n1)
    g1, b1 = finish(1)
    g, b = g0 + g1, b0 + b1
    for i in range(4):
        gb_send[i : i + 1, :] = g[:, i * 128 : (i + 1) * 128]
        gb_send[4 + i : 5 + i, :] = b[:, i * 128 : (i + 1) * 128]

    def gb_copy(j):
        return remote(gb_send, gb_recv.at[j - 1], gb_s.at[j - 1], gb_r.at[j - 1], (me + j) % group)

    for j in range(1, group):
        go(gb_copy(j))
    embed(n1, n2)
    tot = gb_send[...]
    for j in range(1, group):
        gb_copy(j).wait_recv()
        tot = tot + gb_recv[j - 1]
    gain_out[...], bias_out[...] = tot[:4], tot[4:]
    for copy in started:
        copy.wait_send()


def write_out(
    de, loss_in, mean_in, dh_in, gain_in, bias_in,
    loss_out, mean_out, dh_out, de_hbm, gain_out, bias_out,
    sems, *, pieces,
):
    rows = de_hbm.shape[0] // pieces
    half = de_hbm.shape[1] // 2
    copies = []

    def go(src, dst):
        copies.append(pltpu.make_async_copy(src, dst, sems.at[len(copies)]))
        copies[-1].start()

    for i in range(pieces):
        part = pl.ds(i * rows, rows)
        for c in range(2):
            go(de.at[c, part], de_hbm.at[part, pl.ds(c * half, half)])
    for src, dst in ((dh_in, dh_out), (loss_in, loss_out), (gain_in, gain_out), (bias_in, bias_out)):
        go(src, dst)
    mean_out[...] = mean_in[...]
    for copy in copies:
        copy.wait()


def solution(mesh):
    assert mesh.shape["tp"] == 2 * CHIPS

    def group_step(hidden, ln_gain, ln_bias, out_embed, vocab_valid, targets, loss_mask):
        rows, dim = hidden.shape
        vocab = out_embed.shape[0]
        group = 2 * CHIPS
        assert rows == 2 * HT
        vc, ec, n1, n2 = CFG
        nv = vocab // vc
        f32, bf16, i32 = jnp.float32, jnp.bfloat16, jnp.int32
        vmem = pl.BlockSpec(memory_space=pltpu.VMEM)
        hbm = pl.BlockSpec(memory_space=pl.ANY)
        dma = pltpu.SemaphoreType.DMA
        results = pl.pallas_call(
            functools.partial(kernel, vc=vc, ec=ec, n1=n1, n2=n2),
            out_shape=(
                pltpu.VMEM((2, vocab, dim // 2), f32),
                pltpu.VMEM((2, 128), f32),
                pltpu.VMEM((1, 1), f32),
                pltpu.VMEM((rows, dim), bf16),
                pltpu.VMEM((4, 128), f32),
                pltpu.VMEM((4, 128), f32),
            ),
            in_specs=[vmem, vmem, vmem, hbm, vmem, vmem, vmem],
            out_specs=(vmem,) * 6,
            scratch_shapes=[
                pltpu.VMEM((6, vocab, 2 * HT), bf16),
                pltpu.VMEM((2, CHIPS, 2, HT, dim), bf16),
                pltpu.VMEM((SLOTS - 2, vocab, 2 * HT), f32),
                pltpu.VMEM((dim, 2 * HT), bf16),
                pltpu.VMEM((vocab, dim), bf16),
                pltpu.VMEM((nv, dim, vc), bf16),
                pltpu.VMEM((vocab, 128), f32),
                pltpu.VMEM((group, 2, 128), i32),
                pltpu.VMEM((2, 2 * group, 128), f32),
                pltpu.VMEM((2, group - 1, 2 * group, 128), f32),
                pltpu.VMEM((2, group, 128), f32),
                pltpu.VMEM((2, group, 128), f32),
                pltpu.VMEM((2, group, 128), f32),
                pltpu.VMEM((2, CHIPS, 2, dim, HT), f32),
                pltpu.VMEM((2, CHIPS, dim, HT), f32),
                pltpu.VMEM((2, 2, dim // 2, HT), f32),
                pltpu.VMEM((2, 2, dim, HT), f32),
                pltpu.VMEM((8, 128), f32),
                pltpu.VMEM((group - 1, 8, 128), f32),
                pltpu.VMEM((SUB, 128), i32),
                dma((nv,)),
                dma((group - 1,)),
                dma((group - 1,)),
                dma((18,)),
                dma((18,)),
                dma((2 * (group - 1),)),
                dma((2 * (group - 1),)),
                dma((20,)),
                dma((20,)),
                dma((group - 1,)),
                dma((group - 1,)),
            ],
            compiler_params=pltpu.CompilerParams(
                collective_id=0, has_side_effects=True, vmem_limit_bytes=LIM
            ),
            name="vocab_xent",
        )(
            hidden,
            ln_gain.reshape(1, dim),
            ln_bias.reshape(1, dim),
            out_embed,
            vocab_valid.reshape(vocab // 128, 128),
            targets.reshape(2, 128),
            loss_mask.reshape(2, 128),
        )
        loss, mean, dh, de, dgain, dbias = pl.pallas_call(
            functools.partial(write_out, pieces=4),
            out_shape=(
                jax.ShapeDtypeStruct((2, 128), f32),
                jax.ShapeDtypeStruct((1, 1), f32),
                jax.ShapeDtypeStruct((rows, dim), bf16),
                jax.ShapeDtypeStruct((vocab, dim), f32),
                jax.ShapeDtypeStruct((4, 128), f32),
                jax.ShapeDtypeStruct((4, 128), f32),
            ),
            in_specs=[vmem] * 6,
            out_specs=(hbm, vmem, hbm, hbm, hbm, hbm),
            scratch_shapes=[dma((12,))],
            compiler_params=pltpu.CompilerParams(vmem_limit_bytes=2 << 20),
            name="write_out",
        )(*results)
        return (
            loss.reshape(rows),
            mean.reshape(1),
            dh,
            de,
            dgain.reshape(dim),
            dbias.reshape(dim),
        )

    row_spec = P(("dp", "tp"))
    mat_spec = P(("dp", "tp"), None)
    return jax.shard_map(
        group_step,
        mesh=mesh,
        in_specs=(mat_spec, P(None), P(None), P("tp", None), P("tp"), row_spec, row_spec),
        out_specs=(row_spec, P("dp"), mat_spec, mat_spec, P("dp"), P("dp")),
        check_vma=False,
    )
```

```python
import functools

import jax
import jax.numpy as jnp
from jax import lax
from jax.experimental import pallas as pl
from jax.experimental.pallas import tpu as pltpu
from jax.sharding import PartitionSpec as P

SOFT_CAP = 30.0
Z_COEF = 1e-4
LN_EPS = 1e-5
EXP_SCALE = SOFT_CAP * 1.4426950408889634
MESH = pl.DeviceIdType.MESH
CHIPS = 4
OFFSET = (0, 1, 3, 2)
OWN, RIGHT, LEFT, OPP = range(4)
GRADS = ((0, OPP), (0, RIGHT), (0, LEFT), (0, OWN), (1, OPP), (1, RIGHT), (1, LEFT), (1, OWN))
HT = 128
CFG = (512, 512, 6, 8)
FS, BS = 2048, 2048
SLOTS = 6
LIM = 54 * 2**20
SUB = 32

TO_PARTNER, TO_RIGHT, TO_LEFT, FWD_RIGHT, FWD_LEFT, REL_LEFT, REL_RIGHT, REL_OPP_A, REL_OPP_B = range(9)
PAIR, OPP_RIGHT, OPP_LEFT, RIGHT_HI, RIGHT_LO, LEFT_LO, LEFT_HI = 0, 4, 5, 6, 7, 8, 9


def norm(h):
    mean = jnp.mean(h, axis=-1, keepdims=True)
    cent = h - mean
    rstd = lax.rsqrt(jnp.mean(cent * cent, axis=-1, keepdims=True) + LN_EPS)
    return cent * rstd, rstd


def kernel(
    hid, gain, bias, e_hbm, valid, tgt, msk,
    de, loss_out, mean_out, dh_out, gain_out, bias_out,
    dz, x_all, w, xt, e, et, vb, tm_all, st_send, st_recv, av, dv, ls, dx, d2d, ring, fin, gb_send, gb_recv, iota,
    e_sem, tm_s, tm_r, ag_s, ag_r, st_s, st_r, rs_s, rs_r, gb_s, gb_r,
    *, vc, ec, n1, n2,
):
    group = 2 * CHIPS
    me = lax.axis_index("tp")
    c, k = me // 2, me % 2
    other = 1 - k
    partner = 2 * c + other
    chip = [(c + o) % CHIPS for o in OFFSET]
    right, left = 2 * chip[RIGHT] + k, 2 * chip[LEFT] + k
    vocab, dim = e_hbm.shape
    nv = vocab // vc

    def remote(src, dst, send, recv, dev):
        return pltpu.make_async_remote_copy(
            src_ref=src, dst_ref=dst, send_sem=send, recv_sem=recv, device_id={"tp": dev}, device_id_type=MESH
        )

    e_copies = [
        pltpu.make_async_copy(e_hbm.at[pl.ds(i * vc, vc)], e.at[pl.ds(i * vc, vc)], e_sem.at[i]) for i in range(nv)
    ]
    for cp in e_copies:
        cp.start()

    barrier = pltpu.get_barrier_semaphore()
    for j in range(1, group):
        pl.semaphore_signal(barrier, inc=1, device_id={"tp": (me + j) % group}, device_id_type=MESH)

    for h in range(2):
        xh, _ = norm(hid[h * HT : (h + 1) * HT, :].astype(jnp.float32))
        x_all[h, c, k] = (xh * gain[...] + bias[...]).astype(jnp.bfloat16)
    tm_all[me] = tgt[...] * 2 + msk[...]

    pl.semaphore_wait(barrier, group - 1)

    def ag(h, i, src, dst, dev):
        return remote(src, dst, ag_s.at[h * 9 + i], ag_r.at[h * 9 + i], dev)

    def lo(ref):
        return ref.at[pl.ds(0, HT // 2)]

    def hi(ref):
        return ref.at[pl.ds(HT // 2, HT // 2)]

    def block(h, r, core):
        return x_all.at[h, chip[r], core]

    def ag_copy(h, i):
        mine, lft, rgt, opp = block(h, OWN, k), block(h, LEFT, k), block(h, RIGHT, k), block(h, OPP, k)
        src, dev = {
            TO_PARTNER: (mine, partner),
            TO_RIGHT: (mine, right),
            TO_LEFT: (mine, left),
            FWD_RIGHT: (lo(lft), right),
            FWD_LEFT: (hi(rgt), left),
            REL_LEFT: (lft, partner),
            REL_RIGHT: (rgt, partner),
            REL_OPP_A: (lo(opp), partner),
            REL_OPP_B: (hi(opp), partner),
        }[i]
        return ag(h, i, src, src, dev)

    def ag_arrival(h, i):
        ref = {
            TO_PARTNER: block(h, OWN, other),
            TO_RIGHT: block(h, LEFT, k),
            TO_LEFT: block(h, RIGHT, k),
            FWD_RIGHT: lo(block(h, OPP, k)),
            FWD_LEFT: hi(block(h, OPP, k)),
            REL_LEFT: block(h, LEFT, other),
            REL_RIGHT: block(h, RIGHT, other),
            REL_OPP_A: lo(block(h, OPP, other)),
            REL_OPP_B: hi(block(h, OPP, other)),
        }[i]
        ag(h, i, ref, ref, partner).wait_recv()

    started = []

    def go(copy):
        copy.start()
        started.append(copy)

    def tm_copy(j):
        return remote(tm_all.at[me], tm_all.at[me], tm_s.at[j - 1], tm_r.at[j - 1], (me + j) % group)

    for h in range(2):
        if h == 0:
            for j in range(1, group):
                go(tm_copy(j))
        for i in (TO_PARTNER, TO_RIGHT, TO_LEFT):
            go(ag_copy(h, i))

    def tm_arrival(j):
        ref = tm_all.at[(me - j + group) % group]
        remote(ref, ref, tm_s.at[j - 1], tm_r.at[j - 1], partner).wait_recv()

    @pl.loop(0, vocab // 128)
    def _(i):
        row = jnp.broadcast_to(valid[pl.ds(i, 1), :].astype(jnp.float32), (128, 128))
        vb[pl.ds(pl.multiple_of(i * 128, 128), 128), :] = row.T

    for cp in e_copies:
        cp.wait()

    iota[...] = lax.broadcasted_iota(jnp.int32, (SUB, 128), 0)

    def local_target(h, chip_no):
        halves = [
            jnp.broadcast_to((tm_all[2 * chip_no + kk, pl.ds(h, 1), :] >> 1) - me * vocab, (8, 128)) for kk in range(2)
        ]
        return jnp.concatenate(halves, axis=1)

    def weights(slot):
        return de.at[:, pl.ds(slot * 256, 256)] if slot < 2 else w.at[slot - 2]

    def fwd_begin(tiles):
        for n, (h, r, _) in enumerate(tiles):
            xt[:, n * 256 : (n + 1) * 256] = x_all[h, chip[r]].reshape(2 * HT, dim).T
        return [local_target(h, chip[r]) for h, r, _ in tiles]

    def softmax_part(rows0, size, tgts, tiles, carry):
        count = len(tiles)
        z = jnp.dot(e[pl.ds(rows0, size), :], xt[:, : count * 256], preferred_element_type=jnp.float32)
        vb_c = vb.at[pl.ds(rows0, size)]
        outs = [weights(slot).at[pl.ds(rows0, size)] for _, _, slot in tiles]
        carry = list(carry)
        for j in range(size // SUB):
            rows = slice(j * SUB, j * SUB + SUB)
            ok, num = vb_c[rows, :], iota[...]
            ok = jnp.concatenate([ok, ok], axis=1)
            num = jnp.concatenate([num, num], axis=1).reshape(SUB // 8, 8, 256)
            for n in range(count):
                s_acc, t_acc = carry[n]
                t = jnp.tanh(z[rows, n * 256 : (n + 1) * 256] * (1.0 / SOFT_CAP))
                ex = jnp.exp2(t * EXP_SCALE) * ok
                outs[n][rows, :] = ex * (1.0 - t * t)
                hit = num == (tgts[n] - (rows0 + j * SUB))[None]
                s_acc = s_acc + jnp.sum(ex.reshape(SUB // 8, 8, 256), axis=0)
                t_acc = jnp.where(hit, t.reshape(SUB // 8, 8, 256), t_acc)
                carry[n] = s_acc, t_acc
        return tuple(carry)

    def fwd_end(tiles, carry):
        for (h, r, _), (s_acc, t_acc) in zip(tiles, carry):
            s_row = jnp.sum(s_acc, axis=0, keepdims=True)
            t_row = jnp.sum(t_acc.reshape(SUB, 256), axis=0, keepdims=True)
            for kk in range(2):
                st_send[h, pl.ds(2 * chip[r] + kk, 1), :] = s_row[:, kk * 128 : (kk + 1) * 128]
                st_send[h, pl.ds(group + 2 * chip[r] + kk, 1), :] = t_row[:, kk * 128 : (kk + 1) * 128]

    def fwd_zero(tiles):
        zero = (jnp.zeros((8, 256), jnp.float32), jnp.zeros((SUB // 8, 8, 256), jnp.float32))
        return tuple(zero for _ in tiles)

    def forward(*tiles):
        size = FS
        steps = vocab // size
        tgts = fwd_begin(tiles)

        def body(i, carry):
            return softmax_part(pl.multiple_of(i * size, size), size, tgts, tiles, carry)

        fwd_end(tiles, lax.fori_loop(0, steps, body, fwd_zero(tiles)))

    def st_copy(h, j):
        n = h * (group - 1) + j - 1
        return remote(st_send.at[h], st_recv.at[h, j - 1], st_s.at[n], st_r.at[n], (me + j) % group)

    def stats_start(h):
        for j in range(1, group):
            go(st_copy(h, j))

    def token_count():
        total = jnp.zeros((2, 128), jnp.int32)
        for p in range(group):
            total = total + (tm_all[p] & 1)
        total = jnp.sum(jnp.sum(total.astype(jnp.float32), axis=1, keepdims=True), axis=0, keepdims=True)
        return total

    def stats_finish(h):
        tot = st_send[h]
        for j in range(1, group):
            st_copy(h, j).wait_recv()
        for j in range(1, group):
            tot = tot + st_recv[h, j - 1]
        s, t = tot[:group], tot[group:]
        mask = jnp.concatenate([tm_all[p, pl.ds(h, 1), :] & 1 for p in range(group)], axis=0).astype(jnp.float32)
        lse = jnp.log(s)
        coef = mask / token_count()
        a = (1.0 + 2.0 * Z_COEF * lse) * coef / s
        av[h] = a
        dv[h] = (a * jnp.exp2(t * EXP_SCALE) - coef) * (1.0 - t * t)
        ls[h] = (lse - SOFT_CAP * t + Z_COEF * lse * lse) * mask

    def spread(ref, h, chip_no):
        return jnp.concatenate(
            [jnp.broadcast_to(ref[h, pl.ds(2 * chip_no + kk, 1), :], (8, 128)) for kk in range(2)], axis=1
        )

    def bwd_begin(h, r):
        for kk in range(2):
            dx[h, r, kk] = jnp.zeros((dim, HT), jnp.float32)
        return local_target(h, chip[r]), spread(av, h, chip[r]), spread(dv, h, chip[r])

    def grad_store(h, r):
        n = GRADS.index((h, r))
        return dz.at[n] if n < 6 else e.at[:, pl.ds((n - 6) * 256, 256)]

    def hidden_part(i, size, h, r, slot, tgt8, a8, d8):
        rows0 = pl.multiple_of(i * size, size)
        w_c, dz_c = weights(slot).at[pl.ds(rows0, size)], grad_store(h, r).at[pl.ds(rows0, size)]
        part = None
        for u in range(size // vc):
            pieces = []
            for j in range(u * vc // SUB, (u + 1) * vc // SUB):
                rows = slice(j * SUB, j * SUB + SUB)
                num = iota[...]
                hit = jnp.concatenate([num, num], axis=1).reshape(SUB // 8, 8, 256) == (tgt8 - (rows0 + j * SUB))[None]
                g = jnp.where(hit, d8[None], a8[None] * w_c[rows, :].reshape(SUB // 8, 8, 256))
                g = g.reshape(SUB, 256).astype(jnp.bfloat16)
                dz_c[rows, :] = g
                pieces.append(g)
            more = jnp.dot(
                et[i * (size // vc) + u], jnp.concatenate(pieces, axis=0), preferred_element_type=jnp.float32
            )
            part = more if part is None else part + more
        return part

    def bwd_add(h, r, part):
        for kk in range(2):
            dx[h, r, kk] += part[:, kk * HT : (kk + 1) * HT]

    def backward(h, r, slot):
        vecs = bwd_begin(h, r)

        @pl.loop(0, vocab // BS)
        def _(i):
            bwd_add(h, r, hidden_part(i, BS, h, r, slot, *vecs))

    dlo, dhi = pl.ds(0, dim // 2), pl.ds(dim // 2, dim // 2)

    def rs(h, i, src, dst, dev):
        return remote(src, dst, rs_s.at[h * 10 + i], rs_r.at[h * 10 + i], dev)

    def pair_start(h, r):
        go(rs(h, PAIR + r, dx.at[h, r, other], d2d.at[h, r], partner))

    def pair_finish(h, r):
        rs(h, PAIR + r, d2d.at[h, r], d2d.at[h, r], partner).wait_recv()
        dx[h, r, k] = dx[h, r, k] + d2d[h, r]

    def opp_send(h):
        pair_finish(h, OPP)
        go(rs(h, OPP_RIGHT, dx.at[h, OPP, k, dlo], ring.at[h, 0], right))
        go(rs(h, OPP_LEFT, dx.at[h, OPP, k, dhi], ring.at[h, 1], left))

    def right_send(h):
        pair_finish(h, RIGHT)
        go(rs(h, RIGHT_HI, dx.at[h, RIGHT, k, dhi], fin.at[h, 0, dhi], right))

    def left_send(h):
        pair_finish(h, LEFT)
        go(rs(h, LEFT_LO, dx.at[h, LEFT, k, dlo], fin.at[h, 1, dlo], left))

    def ring_right(h):
        rs(h, OPP_RIGHT, ring.at[h, 0], ring.at[h, 0], partner).wait_recv()
        dx[h, RIGHT, k, dlo] = dx[h, RIGHT, k, dlo] + ring[h, 0]
        go(rs(h, RIGHT_LO, dx.at[h, RIGHT, k, dlo], fin.at[h, 0, dlo], right))

    def ring_left(h):
        rs(h, OPP_LEFT, ring.at[h, 1], ring.at[h, 1], partner).wait_recv()
        dx[h, LEFT, k, dhi] = dx[h, LEFT, k, dhi] + ring[h, 1]
        go(rs(h, LEFT_HI, dx.at[h, LEFT, k, dhi], fin.at[h, 1, dhi], left))

    def finish(h):
        for i, n, part in ((RIGHT_HI, 0, dhi), (RIGHT_LO, 0, dlo), (LEFT_LO, 1, dlo), (LEFT_HI, 1, dhi)):
            rs(h, i, fin.at[h, n, part], fin.at[h, n, part], partner).wait_recv()
        dn = (dx[h, OWN, k] + fin[h, 0] + fin[h, 1]).T
        xh, rstd = norm(hid[h * HT : (h + 1) * HT, :].astype(jnp.float32))
        dxh = dn * gain[...]
        m1 = jnp.mean(dxh, axis=-1, keepdims=True)
        m2 = jnp.mean(dxh * xh, axis=-1, keepdims=True)
        dh_out[h * HT : (h + 1) * HT, :] = (rstd * (dxh - m1 - xh * m2)).astype(jnp.bfloat16)
        return jnp.sum(dn * xh, axis=0, keepdims=True), jnp.sum(dn, axis=0, keepdims=True)

    def embed_rows(rows):
        acc = None
        for h in range(2):
            for r in range(CHIPS):
                xx = x_all[h, chip[r]].reshape(2 * HT, dim)
                part = jnp.dot(grad_store(h, r)[rows, :], xx, preferred_element_type=jnp.float32)
                acc = part if acc is None else acc + part
        return acc

    def embed(first, last):
        @pl.loop(first, last)
        def _(i):
            rows = pl.ds(pl.multiple_of(i * ec, ec), ec)
            de[rows, :] = embed_rows(rows)

    jp = 6 - 6 * k
    ref0 = tm_all.at[0]

    def ag_pass(h):
        ag_arrival(h, TO_RIGHT)
        ag_arrival(h, TO_LEFT)
        for i in (FWD_RIGHT, FWD_LEFT, REL_RIGHT, REL_LEFT):
            go(ag_copy(h, i))

    def ag_pass_opp(h):
        ag_arrival(h, FWD_RIGHT)
        ag_arrival(h, FWD_LEFT)
        for i in (REL_OPP_A, REL_OPP_B):
            go(ag_copy(h, i))

    remote(ref0, ref0, tm_s.at[jp], tm_r.at[jp], partner).wait_recv()
    ag_arrival(0, TO_PARTNER)
    ag_arrival(1, TO_PARTNER)
    forward((0, OWN, 0))
    forward((1, OWN, 1))
    for i in range(1, group - 1):
        n = (jp + i) % (group - 1)
        remote(ref0, ref0, tm_s.at[n], tm_r.at[n], partner).wait_recv()
    ag_pass(0)

    @pl.loop(0, nv)
    def _(i):
        et[i] = e[pl.ds(pl.multiple_of(i * vc, vc), vc), :].T

    ag_arrival(0, REL_RIGHT)
    forward((0, RIGHT, 2))
    ag_pass(1)
    ag_pass_opp(0)
    ag_arrival(0, REL_LEFT)
    forward((0, LEFT, 3))
    ag_arrival(0, REL_OPP_A)
    ag_arrival(0, REL_OPP_B)
    forward((0, OPP, 4))
    stats_start(0)
    ag_pass_opp(1)
    ag_arrival(1, REL_RIGHT)
    forward((1, RIGHT, 5))
    stats_finish(0)
    ag_arrival(1, REL_LEFT)
    backward(0, OPP, 4)
    pair_start(0, OPP)
    backward(0, RIGHT, 2)
    pair_start(0, RIGHT)
    opp_send(0)
    forward((1, LEFT, 4))
    right_send(0)
    ag_arrival(1, REL_OPP_A)
    ag_arrival(1, REL_OPP_B)
    forward((1, OPP, 2))
    stats_start(1)
    backward(0, LEFT, 3)
    pair_start(0, LEFT)
    ring_right(0)
    backward(0, OWN, 0)
    pair_start(0, OWN)
    left_send(0)
    ring_left(0)
    stats_finish(1)
    loss_out[...] = jnp.concatenate([ls[h, pl.ds(me, 1), :] for h in range(2)], axis=0)
    total = ls[0] + ls[1]
    mean_out[...] = jnp.sum(jnp.sum(total, axis=1, keepdims=True), axis=0, keepdims=True) / token_count()
    backward(1, OPP, 2)
    pair_start(1, OPP)
    backward(1, RIGHT, 5)
    pair_start(1, RIGHT)
    opp_send(1)
    backward(1, LEFT, 4)
    pair_start(1, LEFT)
    right_send(1)
    backward(1, OWN, 1)
    pair_start(1, OWN)
    left_send(1)
    embed(0, 2)
    ring_right(1)
    ring_left(1)
    pair_finish(0, OWN)
    pair_finish(1, OWN)
    g0, b0 = finish(0)
    embed(2, n1)
    g1, b1 = finish(1)
    g, b = g0 + g1, b0 + b1
    for i in range(4):
        gb_send[i : i + 1, :] = g[:, i * 128 : (i + 1) * 128]
        gb_send[4 + i : 5 + i, :] = b[:, i * 128 : (i + 1) * 128]

    def gb_copy(j):
        return remote(gb_send, gb_recv.at[j - 1], gb_s.at[j - 1], gb_r.at[j - 1], (me + j) % group)

    for j in range(1, group):
        go(gb_copy(j))
    embed(n1, n2)
    tot = gb_send[...]
    for j in range(1, group):
        gb_copy(j).wait_recv()
        tot = tot + gb_recv[j - 1]
    gain_out[...], bias_out[...] = tot[:4], tot[4:]
    for copy in started:
        copy.wait_send()


def write_out(
    de, loss_in, mean_in, dh_in, gain_in, bias_in,
    loss_out, mean_out, dh_out, de_hbm, gain_out, bias_out,
    sems, *, pieces,
):
    rows = de_hbm.shape[0] // pieces
    copies = []

    def go(src, dst):
        copies.append(pltpu.make_async_copy(src, dst, sems.at[len(copies)]))
        copies[-1].start()

    for i in range(pieces):
        part = pl.ds(i * rows, rows)
        go(de.at[part], de_hbm.at[part])
    for src, dst in ((dh_in, dh_out), (loss_in, loss_out), (gain_in, gain_out), (bias_in, bias_out)):
        go(src, dst)
    mean_out[...] = mean_in[...]
    for copy in copies:
        copy.wait()


def solution(mesh):
    assert mesh.shape["tp"] == 2 * CHIPS

    def group_step(hidden, ln_gain, ln_bias, out_embed, vocab_valid, targets, loss_mask):
        rows, dim = hidden.shape
        vocab = out_embed.shape[0]
        group = 2 * CHIPS
        assert rows == 2 * HT
        vc, ec, n1, n2 = CFG
        nv = vocab // vc
        f32, bf16, i32 = jnp.float32, jnp.bfloat16, jnp.int32
        vmem = pl.BlockSpec(memory_space=pltpu.VMEM)
        hbm = pl.BlockSpec(memory_space=pl.ANY)
        dma = pltpu.SemaphoreType.DMA
        results = pl.pallas_call(
            functools.partial(kernel, vc=vc, ec=ec, n1=n1, n2=n2),
            out_shape=(
                pltpu.VMEM((vocab, dim), f32),
                pltpu.VMEM((2, 128), f32),
                pltpu.VMEM((1, 1), f32),
                pltpu.VMEM((rows, dim), bf16),
                pltpu.VMEM((4, 128), f32),
                pltpu.VMEM((4, 128), f32),
            ),
            in_specs=[vmem, vmem, vmem, hbm, vmem, vmem, vmem],
            out_specs=(vmem,) * 6,
            scratch_shapes=[
                pltpu.VMEM((6, vocab, 2 * HT), bf16),
                pltpu.VMEM((2, CHIPS, 2, HT, dim), bf16),
                pltpu.VMEM((SLOTS - 2, vocab, 2 * HT), f32),
                pltpu.VMEM((dim, 2 * HT), bf16),
                pltpu.VMEM((vocab, dim), bf16),
                pltpu.VMEM((nv, dim, vc), bf16),
                pltpu.VMEM((vocab, 128), f32),
                pltpu.VMEM((group, 2, 128), i32),
                pltpu.VMEM((2, 2 * group, 128), f32),
                pltpu.VMEM((2, group - 1, 2 * group, 128), f32),
                pltpu.VMEM((2, group, 128), f32),
                pltpu.VMEM((2, group, 128), f32),
                pltpu.VMEM((2, group, 128), f32),
                pltpu.VMEM((2, CHIPS, 2, dim, HT), f32),
                pltpu.VMEM((2, CHIPS, dim, HT), f32),
                pltpu.VMEM((2, 2, dim // 2, HT), f32),
                pltpu.VMEM((2, 2, dim, HT), f32),
                pltpu.VMEM((8, 128), f32),
                pltpu.VMEM((group - 1, 8, 128), f32),
                pltpu.VMEM((SUB, 128), i32),
                dma((nv,)),
                dma((group - 1,)),
                dma((group - 1,)),
                dma((18,)),
                dma((18,)),
                dma((2 * (group - 1),)),
                dma((2 * (group - 1),)),
                dma((20,)),
                dma((20,)),
                dma((group - 1,)),
                dma((group - 1,)),
            ],
            compiler_params=pltpu.CompilerParams(
                collective_id=0, has_side_effects=True, vmem_limit_bytes=LIM
            ),
            name="vocab_xent",
        )(
            hidden,
            ln_gain.reshape(1, dim),
            ln_bias.reshape(1, dim),
            out_embed,
            vocab_valid.reshape(vocab // 128, 128),
            targets.reshape(2, 128),
            loss_mask.reshape(2, 128),
        )
        loss, mean, dh, de, dgain, dbias = pl.pallas_call(
            functools.partial(write_out, pieces=8),
            out_shape=(
                jax.ShapeDtypeStruct((2, 128), f32),
                jax.ShapeDtypeStruct((1, 1), f32),
                jax.ShapeDtypeStruct((rows, dim), bf16),
                jax.ShapeDtypeStruct((vocab, dim), f32),
                jax.ShapeDtypeStruct((4, 128), f32),
                jax.ShapeDtypeStruct((4, 128), f32),
            ),
            in_specs=[vmem] * 6,
            out_specs=(hbm, vmem, hbm, hbm, hbm, hbm),
            scratch_shapes=[dma((12,))],
            compiler_params=pltpu.CompilerParams(vmem_limit_bytes=2 << 20),
            name="write_out",
        )(*results)
        return (
            loss.reshape(rows),
            mean.reshape(1),
            dh,
            de,
            dgain.reshape(dim),
            dbias.reshape(dim),
        )

    row_spec = P(("dp", "tp"))
    mat_spec = P(("dp", "tp"), None)
    return jax.shard_map(
        group_step,
        mesh=mesh,
        in_specs=(mat_spec, P(None), P(None), P("tp", None), P("tp"), row_spec, row_spec),
        out_specs=(row_spec, P("dp"), mat_spec, mat_spec, P("dp"), P("dp")),
        check_vma=False,
    )
```

```python
import functools

import jax
import jax.numpy as jnp
from jax import lax
from jax.experimental import pallas as pl
from jax.experimental.pallas import tpu as pltpu
from jax.sharding import PartitionSpec as P

SOFT_CAP = 30.0
Z_COEF = 1e-4
LN_EPS = 1e-5
EXP_SCALE = SOFT_CAP * 1.4426950408889634
MESH = pl.DeviceIdType.MESH
CHIPS = 4
OFFSET = (0, 1, 3, 2)
OWN, RIGHT, LEFT, OPP = range(4)
GRADS = ((0, OPP), (0, RIGHT), (0, LEFT), (0, OWN), (1, OPP), (1, RIGHT), (1, LEFT), (1, OWN))
HT = 128
CFG = (512, 512, 5, 8)
FS, FD, BS, DOT = 2048, 2048, 2048, 128
SLOTS = 6
LIM = 54 * 2**20
SUB = 32

TO_PARTNER, TO_RIGHT, TO_LEFT, FWD_RIGHT, FWD_LEFT, REL_LEFT, REL_RIGHT, REL_OPP_A, REL_OPP_B = range(9)
PAIR, OPP_RIGHT, OPP_LEFT, RIGHT_HI, RIGHT_LO, LEFT_LO, LEFT_HI = 0, 4, 5, 6, 7, 8, 9


def norm(h):
    mean = jnp.mean(h, axis=-1, keepdims=True)
    cent = h - mean
    rstd = lax.rsqrt(jnp.mean(cent * cent, axis=-1, keepdims=True) + LN_EPS)
    return cent * rstd, rstd


def kernel(
    hid_hbm, gain_hbm, bias_hbm, e_hbm, valid_hbm, tgt_hbm, msk_hbm,
    de, loss_out, dh_out, gain_out, bias_out,
    hid, gain, bias, valid, tgt, msk, in_sem,
    dz, x_all, w, xt, e, et, vb, tm_all, st_send, st_recv, av, dv, ls, dx, d2d, ring, fin, gb_send, gb_recv, iota,
    e_sem, tm_s, tm_r, ag_s, ag_r, st_s, st_r, rs_s, rs_r, gb_s, gb_r,
    *, vc, ec, n1, n2,
):
    group = 2 * CHIPS
    me = lax.axis_index("tp")
    c, k = me // 2, me % 2
    other = 1 - k
    partner = 2 * c + other
    chip = [(c + o) % CHIPS for o in OFFSET]
    right, left = 2 * chip[RIGHT] + k, 2 * chip[LEFT] + k
    vocab, dim = e_hbm.shape
    nv = vocab // vc

    def remote(src, dst, send, recv, dev):
        return pltpu.make_async_remote_copy(
            src_ref=src, dst_ref=dst, send_sem=send, recv_sem=recv, device_id={"tp": dev}, device_id_type=MESH
        )

    barrier = pltpu.get_barrier_semaphore()
    for j in range(1, group):
        pl.semaphore_signal(barrier, inc=1, device_id={"tp": (me + j) % group}, device_id_type=MESH)

    pairs = ((hid_hbm, hid), (gain_hbm, gain), (bias_hbm, bias), (tgt_hbm, tgt), (msk_hbm, msk), (valid_hbm, valid))
    inputs = [pltpu.make_async_copy(src, dst, in_sem.at[i]) for i, (src, dst) in enumerate(pairs)]
    for cp in inputs:
        cp.start()
    e_copies = [
        pltpu.make_async_copy(e_hbm.at[pl.ds(i * vc, vc)], e.at[pl.ds(i * vc, vc)], e_sem.at[i]) for i in range(nv)
    ]
    for cp in e_copies:
        cp.start()

    for cp in inputs[:5]:
        cp.wait()

    for h in range(2):
        xh, _ = norm(hid[h * HT : (h + 1) * HT, :].astype(jnp.float32))
        x_all[h, c, k] = (xh * gain[...] + bias[...]).astype(jnp.bfloat16)
    tm_all[me] = tgt[...] * 2 + msk[...]

    pl.semaphore_wait(barrier, group - 1)

    def ag(h, i, src, dst, dev):
        return remote(src, dst, ag_s.at[h * 9 + i], ag_r.at[h * 9 + i], dev)

    def lo(ref):
        return ref.at[pl.ds(0, HT // 2)]

    def hi(ref):
        return ref.at[pl.ds(HT // 2, HT // 2)]

    def block(h, r, core):
        return x_all.at[h, chip[r], core]

    def ag_copy(h, i):
        mine, lft, rgt, opp = block(h, OWN, k), block(h, LEFT, k), block(h, RIGHT, k), block(h, OPP, k)
        src, dev = {
            TO_PARTNER: (mine, partner),
            TO_RIGHT: (mine, right),
            TO_LEFT: (mine, left),
            FWD_RIGHT: (lo(lft), right),
            FWD_LEFT: (hi(rgt), left),
            REL_LEFT: (lft, partner),
            REL_RIGHT: (rgt, partner),
            REL_OPP_A: (lo(opp), partner),
            REL_OPP_B: (hi(opp), partner),
        }[i]
        return ag(h, i, src, src, dev)

    def ag_arrival(h, i):
        ref = {
            TO_PARTNER: block(h, OWN, other),
            TO_RIGHT: block(h, LEFT, k),
            TO_LEFT: block(h, RIGHT, k),
            FWD_RIGHT: lo(block(h, OPP, k)),
            FWD_LEFT: hi(block(h, OPP, k)),
            REL_LEFT: block(h, LEFT, other),
            REL_RIGHT: block(h, RIGHT, other),
            REL_OPP_A: lo(block(h, OPP, other)),
            REL_OPP_B: hi(block(h, OPP, other)),
        }[i]
        ag(h, i, ref, ref, partner).wait_recv()

    started = []

    def go(make, *args):
        make(*args).start()
        started.append((make, args))

    def tm_copy(j):
        return remote(tm_all.at[me], tm_all.at[me], tm_s.at[j - 1], tm_r.at[j - 1], (me + j) % group)

    for h in range(2):
        if h == 0:
            for j in range(1, group):
                go(tm_copy, j)
        for i in (TO_PARTNER, TO_RIGHT, TO_LEFT):
            go(ag_copy, h, i)

    def tm_arrival(j):
        ref = tm_all.at[(me - j + group) % group]
        remote(ref, ref, tm_s.at[j - 1], tm_r.at[j - 1], partner).wait_recv()

    inputs[5].wait()

    @pl.loop(0, vocab // 128)
    def _(i):
        row = jnp.broadcast_to(valid[pl.ds(i, 1), :].astype(jnp.float32), (128, 128))
        vb[pl.ds(pl.multiple_of(i * 128, 128), 128), :] = row.T

    for cp in e_copies:
        cp.wait()

    iota[...] = lax.broadcasted_iota(jnp.int32, (SUB, 128), 0)

    def local_target(h, chip_no):
        halves = [
            jnp.broadcast_to((tm_all[2 * chip_no + kk, pl.ds(h, 1), :] >> 1) - me * vocab, (8, 128)) for kk in range(2)
        ]
        return jnp.concatenate(halves, axis=1)

    def weights(slot):
        return de.at[:, pl.ds(slot * 256, 256)] if slot < 2 else w.at[slot - 2]

    def fwd_begin(tiles):
        for n, (h, r, _) in enumerate(tiles):
            xt[:, n * 256 : (n + 1) * 256] = x_all[h, chip[r]].reshape(2 * HT, dim).T
        return [local_target(h, chip[r]) for h, r, _ in tiles]

    def softmax_part(rows0, size, tgts, tiles, carry):
        count = len(tiles)
        e_c = e.at[pl.ds(rows0, size)]
        vb_c = vb.at[pl.ds(rows0, size)]
        outs = [weights(slot).at[pl.ds(rows0, size)] for _, _, slot in tiles]
        carry = list(carry)
        for j in range(size // SUB):
            if j % (DOT // SUB) == 0:
                z = jnp.dot(
                    e_c[j * SUB : j * SUB + DOT, :], xt[:, : count * 256], preferred_element_type=jnp.float32
                )
            rows = slice(j * SUB, j * SUB + SUB)
            part = slice(j * SUB % DOT, j * SUB % DOT + SUB)
            ok, num = vb_c[rows, :], iota[...]
            ok = jnp.concatenate([ok, ok], axis=1)
            num = jnp.concatenate([num, num], axis=1).reshape(SUB // 8, 8, 256)
            for n in range(count):
                s_acc, t_acc = carry[n]
                t = jnp.tanh(z[part, n * 256 : (n + 1) * 256] * (1.0 / SOFT_CAP))
                ex = jnp.exp2(t * EXP_SCALE) * ok
                outs[n][rows, :] = ex * (1.0 - t * t)
                hit = num == (tgts[n] - (rows0 + j * SUB))[None]
                s_acc = s_acc + jnp.sum(ex.reshape(SUB // 8, 8, 256), axis=0)
                t_acc = jnp.where(hit, t.reshape(SUB // 8, 8, 256), t_acc)
                carry[n] = s_acc, t_acc
        return tuple(carry)

    def fwd_end(tiles, carry):
        for (h, r, _), (s_acc, t_acc) in zip(tiles, carry):
            s_row = jnp.sum(s_acc, axis=0, keepdims=True)
            t_row = jnp.sum(t_acc.reshape(SUB, 256), axis=0, keepdims=True)
            for kk in range(2):
                st_send[h, pl.ds(2 * chip[r] + kk, 1), :] = s_row[:, kk * 128 : (kk + 1) * 128]
                st_send[h, pl.ds(group + 2 * chip[r] + kk, 1), :] = t_row[:, kk * 128 : (kk + 1) * 128]

    def fwd_zero(tiles):
        zero = (jnp.zeros((8, 256), jnp.float32), jnp.zeros((SUB // 8, 8, 256), jnp.float32))
        return tuple(zero for _ in tiles)

    def forward(*tiles, halfway=None):
        size = FS if len(tiles) == 1 else FD
        steps = vocab // size
        tgts = fwd_begin(tiles)

        def body(i, carry):
            if halfway is not None:

                @pl.when(i == steps // 2)
                def _():
                    halfway()

            return softmax_part(pl.multiple_of(i * size, size), size, tgts, tiles, carry)

        fwd_end(tiles, lax.fori_loop(0, steps, body, fwd_zero(tiles)))

    def st_copy(h, j):
        n = h * (group - 1) + j - 1
        return remote(st_send.at[h], st_recv.at[h, j - 1], st_s.at[n], st_r.at[n], (me + j) % group)

    def stats_start(h):
        for j in range(1, group):
            go(st_copy, h, j)

    def token_count():
        total = jnp.zeros((2, 128), jnp.int32)
        for p in range(group):
            total = total + (tm_all[p] & 1)
        total = jnp.sum(jnp.sum(total.astype(jnp.float32), axis=1, keepdims=True), axis=0, keepdims=True)
        return total

    def stats_finish(h):
        tot = st_send[h]
        for j in range(1, group):
            st_copy(h, j).wait_recv()
        for j in range(1, group):
            tot = tot + st_recv[h, j - 1]
        s, t = tot[:group], tot[group:]
        mask = jnp.concatenate([tm_all[p, pl.ds(h, 1), :] & 1 for p in range(group)], axis=0).astype(jnp.float32)
        lse = jnp.log(s)
        coef = mask / token_count()
        a = (1.0 + 2.0 * Z_COEF * lse) * coef / s
        av[h] = a
        dv[h] = (a * jnp.exp2(t * EXP_SCALE) - coef) * (1.0 - t * t)
        ls[h] = (lse - SOFT_CAP * t + Z_COEF * lse * lse) * mask

    def spread(ref, h, chip_no):
        return jnp.concatenate(
            [jnp.broadcast_to(ref[h, pl.ds(2 * chip_no + kk, 1), :], (8, 128)) for kk in range(2)], axis=1
        )

    def bwd_begin(h, r):
        for kk in range(2):
            dx[h, r, kk] = jnp.zeros((dim, HT), jnp.float32)
        return local_target(h, chip[r]), spread(av, h, chip[r]), spread(dv, h, chip[r])

    def grad_store(h, r):
        n = GRADS.index((h, r))
        return dz.at[n] if n < 6 else e.at[:, pl.ds((n - 6) * 256, 256)]

    def hidden_part(i, size, h, r, slot, tgt8, a8, d8):
        rows0 = pl.multiple_of(i * size, size)
        w_c, dz_c = weights(slot).at[pl.ds(rows0, size)], grad_store(h, r).at[pl.ds(rows0, size)]
        part = None
        for u in range(size // vc):
            pieces = []
            for j in range(u * vc // SUB, (u + 1) * vc // SUB):
                rows = slice(j * SUB, j * SUB + SUB)
                num = iota[...]
                hit = jnp.concatenate([num, num], axis=1).reshape(SUB // 8, 8, 256) == (tgt8 - (rows0 + j * SUB))[None]
                g = jnp.where(hit, d8[None], a8[None] * w_c[rows, :].reshape(SUB // 8, 8, 256))
                g = g.reshape(SUB, 256).astype(jnp.bfloat16)
                dz_c[rows, :] = g
                pieces.append(g)
            more = jnp.dot(
                et[i * (size // vc) + u], jnp.concatenate(pieces, axis=0), preferred_element_type=jnp.float32
            )
            part = more if part is None else part + more
        return part

    def bwd_add(h, r, part):
        for kk in range(2):
            dx[h, r, kk] += part[:, kk * HT : (kk + 1) * HT]

    def backward(h, r, slot):
        vecs = bwd_begin(h, r)

        @pl.loop(0, vocab // BS)
        def _(i):
            bwd_add(h, r, hidden_part(i, BS, h, r, slot, *vecs))

    dlo, dhi = pl.ds(0, dim // 2), pl.ds(dim // 2, dim // 2)

    def rs(h, i, src, dst, dev):
        return remote(src, dst, rs_s.at[h * 10 + i], rs_r.at[h * 10 + i], dev)

    def pair_start(h, r):
        go(lambda: rs(h, PAIR + r, dx.at[h, r, other], d2d.at[h, r], partner))

    def pair_finish(h, r):
        rs(h, PAIR + r, d2d.at[h, r], d2d.at[h, r], partner).wait_recv()
        dx[h, r, k] = dx[h, r, k] + d2d[h, r]

    def opp_send(h):
        pair_finish(h, OPP)
        go(lambda: rs(h, OPP_RIGHT, dx.at[h, OPP, k, dlo], ring.at[h, 0], right))
        go(lambda: rs(h, OPP_LEFT, dx.at[h, OPP, k, dhi], ring.at[h, 1], left))

    def right_send(h):
        pair_finish(h, RIGHT)
        go(lambda: rs(h, RIGHT_HI, dx.at[h, RIGHT, k, dhi], fin.at[h, 0, dhi], right))

    def left_send(h):
        pair_finish(h, LEFT)
        go(lambda: rs(h, LEFT_LO, dx.at[h, LEFT, k, dlo], fin.at[h, 1, dlo], left))

    def ring_right(h):
        rs(h, OPP_RIGHT, ring.at[h, 0], ring.at[h, 0], partner).wait_recv()
        dx[h, RIGHT, k, dlo] = dx[h, RIGHT, k, dlo] + ring[h, 0]
        go(lambda: rs(h, RIGHT_LO, dx.at[h, RIGHT, k, dlo], fin.at[h, 0, dlo], right))

    def ring_left(h):
        rs(h, OPP_LEFT, ring.at[h, 1], ring.at[h, 1], partner).wait_recv()
        dx[h, LEFT, k, dhi] = dx[h, LEFT, k, dhi] + ring[h, 1]
        go(lambda: rs(h, LEFT_HI, dx.at[h, LEFT, k, dhi], fin.at[h, 1, dhi], left))

    def finish(h):
        for i, n, part in ((RIGHT_HI, 0, dhi), (RIGHT_LO, 0, dlo), (LEFT_LO, 1, dlo), (LEFT_HI, 1, dhi)):
            rs(h, i, fin.at[h, n, part], fin.at[h, n, part], partner).wait_recv()
        dn = (dx[h, OWN, k] + fin[h, 0] + fin[h, 1]).T
        xh, rstd = norm(hid[h * HT : (h + 1) * HT, :].astype(jnp.float32))
        dxh = dn * gain[...]
        m1 = jnp.mean(dxh, axis=-1, keepdims=True)
        m2 = jnp.mean(dxh * xh, axis=-1, keepdims=True)
        dh_out[h * HT : (h + 1) * HT, :] = (rstd * (dxh - m1 - xh * m2)).astype(jnp.bfloat16)
        return jnp.sum(dn * xh, axis=0, keepdims=True), jnp.sum(dn, axis=0, keepdims=True)

    def embed_rows(rows):
        acc = None
        for h in range(2):
            for r in range(CHIPS):
                xx = x_all[h, chip[r]].reshape(2 * HT, dim)
                part = jnp.dot(grad_store(h, r)[rows, :], xx, preferred_element_type=jnp.float32)
                acc = part if acc is None else acc + part
        return acc

    def embed(first, last):
        @pl.loop(first, last)
        def _(i):
            rows = pl.ds(pl.multiple_of(i * ec, ec), ec)
            de[rows, :] = embed_rows(rows)

    jp = 6 - 6 * k
    ref0 = tm_all.at[0]

    def ag_pass(h):
        ag_arrival(h, TO_RIGHT)
        ag_arrival(h, TO_LEFT)
        for i in (FWD_RIGHT, FWD_LEFT, REL_RIGHT, REL_LEFT):
            go(ag_copy, h, i)

    def ag_pass_opp(h):
        ag_arrival(h, FWD_RIGHT)
        ag_arrival(h, FWD_LEFT)
        for i in (REL_OPP_A, REL_OPP_B):
            go(ag_copy, h, i)

    remote(ref0, ref0, tm_s.at[jp], tm_r.at[jp], partner).wait_recv()
    ag_arrival(0, TO_PARTNER)
    ag_arrival(1, TO_PARTNER)
    forward((0, OWN, 0), (1, OWN, 1))
    for i in range(1, group - 1):
        n = (jp + i) % (group - 1)
        remote(ref0, ref0, tm_s.at[n], tm_r.at[n], partner).wait_recv()
    ag_pass(0)

    @pl.loop(0, nv)
    def _(i):
        et[i] = e[pl.ds(pl.multiple_of(i * vc, vc), vc), :].T

    ag_arrival(0, REL_RIGHT)
    forward((0, RIGHT, 2))
    ag_pass(1)
    ag_pass_opp(0)
    ag_arrival(0, REL_LEFT)
    forward((0, LEFT, 3))
    ag_arrival(0, REL_OPP_A)
    ag_arrival(0, REL_OPP_B)
    forward((0, OPP, 4))
    stats_start(0)
    ag_pass_opp(1)
    ag_arrival(1, REL_RIGHT)
    forward((1, RIGHT, 5))
    stats_finish(0)
    ag_arrival(1, REL_LEFT)
    backward(0, OPP, 4)
    pair_start(0, OPP)
    backward(0, RIGHT, 2)
    pair_start(0, RIGHT)
    opp_send(0)
    ag_arrival(1, REL_OPP_A)
    ag_arrival(1, REL_OPP_B)
    forward((1, LEFT, 4), (1, OPP, 2), halfway=lambda: right_send(0))
    stats_start(1)
    backward(0, LEFT, 3)
    pair_start(0, LEFT)
    ring_right(0)
    backward(0, OWN, 0)
    pair_start(0, OWN)
    left_send(0)
    ring_left(0)
    stats_finish(1)
    for h in range(2):
        loss_out[h : h + 1, :] = ls[h, pl.ds(me, 1), :]
    total = ls[0] + ls[1]
    mean = jnp.sum(jnp.sum(total, axis=1, keepdims=True), axis=0, keepdims=True) / token_count()
    loss_out[2:, :] = jnp.broadcast_to(mean, (6, 128))
    backward(1, OPP, 2)
    pair_start(1, OPP)
    backward(1, RIGHT, 5)
    pair_start(1, RIGHT)
    opp_send(1)
    backward(1, LEFT, 4)
    pair_start(1, LEFT)
    right_send(1)
    backward(1, OWN, 1)
    pair_start(1, OWN)
    left_send(1)
    embed(0, 2)
    ring_right(1)
    ring_left(1)
    pair_finish(0, OWN)
    pair_finish(1, OWN)
    g0, b0 = finish(0)
    embed(2, n1)
    g1, b1 = finish(1)
    g, b = g0 + g1, b0 + b1
    for i in range(4):
        gb_send[i : i + 1, :] = g[:, i * 128 : (i + 1) * 128]
        gb_send[4 + i : 5 + i, :] = b[:, i * 128 : (i + 1) * 128]

    def gb_copy(j):
        return remote(gb_send, gb_recv.at[j - 1], gb_s.at[j - 1], gb_r.at[j - 1], (me + j) % group)

    for j in range(1, group):
        go(gb_copy, j)
    embed(n1, n2)
    tot = gb_send[...]
    for j in range(1, group):
        gb_copy(j).wait_recv()
        tot = tot + gb_recv[j - 1]
    gain_out[...], bias_out[...] = tot[:4], tot[4:]
    for make, args in started:
        make(*args).wait_send()


def write_out(
    de, loss_in, dh_in, gain_in, bias_in,
    loss_out, mean_out, dh_out, de_hbm, gain_out, bias_out,
    loss, mean, sems, *, pieces,
):
    rows = de_hbm.shape[0] // pieces
    copies = []

    def go(src, dst):
        copies.append(pltpu.make_async_copy(src, dst, sems.at[len(copies)]))
        copies[-1].start()

    for i in range(pieces):
        part = pl.ds(i * rows, rows)
        go(de.at[part], de_hbm.at[part])
    loss[...] = loss_in[0:2, :]
    mean[...] = loss_in[2:3, 0:1]
    for src, dst in ((dh_in, dh_out), (gain_in, gain_out), (bias_in, bias_out), (loss, loss_out), (mean, mean_out)):
        go(src, dst)
    for copy in copies:
        copy.wait()


def solution(mesh):
    assert mesh.shape["tp"] == 2 * CHIPS

    def group_step(hidden, ln_gain, ln_bias, out_embed, vocab_valid, targets, loss_mask):
        rows, dim = hidden.shape
        vocab = out_embed.shape[0]
        group = 2 * CHIPS
        assert rows == 2 * HT
        vc, ec, n1, n2 = CFG
        nv = vocab // vc
        f32, bf16, i32 = jnp.float32, jnp.bfloat16, jnp.int32
        vmem = pl.BlockSpec(memory_space=pltpu.VMEM)
        hbm = pl.BlockSpec(memory_space=pl.ANY)
        dma = pltpu.SemaphoreType.DMA
        results = pl.pallas_call(
            functools.partial(kernel, vc=vc, ec=ec, n1=n1, n2=n2),
            out_shape=(
                pltpu.VMEM((vocab, dim), f32),
                pltpu.VMEM((8, 128), f32),
                pltpu.VMEM((rows, dim), bf16),
                pltpu.VMEM((4, 128), f32),
                pltpu.VMEM((4, 128), f32),
            ),
            in_specs=[hbm] * 7,
            out_specs=(vmem,) * 5,
            scratch_shapes=[
                pltpu.VMEM((rows, dim), bf16),
                pltpu.VMEM((1, dim), f32),
                pltpu.VMEM((1, dim), f32),
                pltpu.VMEM((vocab // 128, 128), i32),
                pltpu.VMEM((2, 128), i32),
                pltpu.VMEM((2, 128), i32),
                dma((6,)),
                pltpu.VMEM((6, vocab, 2 * HT), bf16),
                pltpu.VMEM((2, CHIPS, 2, HT, dim), bf16),
                pltpu.VMEM((SLOTS - 2, vocab, 2 * HT), f32),
                pltpu.VMEM((dim, 4 * HT), bf16),
                pltpu.VMEM((vocab, dim), bf16),
                pltpu.VMEM((nv, dim, vc), bf16),
                pltpu.VMEM((vocab, 128), f32),
                pltpu.VMEM((group, 2, 128), i32),
                pltpu.VMEM((2, 2 * group, 128), f32),
                pltpu.VMEM((2, group - 1, 2 * group, 128), f32),
                pltpu.VMEM((2, group, 128), f32),
                pltpu.VMEM((2, group, 128), f32),
                pltpu.VMEM((2, group, 128), f32),
                pltpu.VMEM((2, CHIPS, 2, dim, HT), f32),
                pltpu.VMEM((2, CHIPS, dim, HT), f32),
                pltpu.VMEM((2, 2, dim // 2, HT), f32),
                pltpu.VMEM((2, 2, dim, HT), f32),
                pltpu.VMEM((8, 128), f32),
                pltpu.VMEM((group - 1, 8, 128), f32),
                pltpu.VMEM((SUB, 128), i32),
                dma((nv,)),
                dma((group - 1,)),
                dma((group - 1,)),
                dma((18,)),
                dma((18,)),
                dma((2 * (group - 1),)),
                dma((2 * (group - 1),)),
                dma((20,)),
                dma((20,)),
                dma((group - 1,)),
                dma((group - 1,)),
            ],
            compiler_params=pltpu.CompilerParams(
                collective_id=0, has_side_effects=True, vmem_limit_bytes=LIM
            ),
            name="vocab_xent",
        )(
            hidden,
            ln_gain.reshape(1, dim),
            ln_bias.reshape(1, dim),
            out_embed,
            vocab_valid.reshape(vocab // 128, 128),
            targets.reshape(2, 128),
            loss_mask.reshape(2, 128),
        )
        loss, mean, dh, de, dgain, dbias = pl.pallas_call(
            functools.partial(write_out, pieces=8),
            out_shape=(
                jax.ShapeDtypeStruct((2, 128), f32),
                jax.ShapeDtypeStruct((1, 1), f32),
                jax.ShapeDtypeStruct((rows, dim), bf16),
                jax.ShapeDtypeStruct((vocab, dim), f32),
                jax.ShapeDtypeStruct((4, 128), f32),
                jax.ShapeDtypeStruct((4, 128), f32),
            ),
            in_specs=[vmem] * 5,
            out_specs=(hbm,) * 6,
            scratch_shapes=[pltpu.VMEM((2, 128), f32), pltpu.VMEM((1, 1), f32), dma((13,))],
            compiler_params=pltpu.CompilerParams(vmem_limit_bytes=2 << 20),
            name="write_out",
        )(*results)
        return (
            loss.reshape(rows),
            mean.reshape(1),
            dh,
            de,
            dgain.reshape(dim),
            dbias.reshape(dim),
        )

    row_spec = P(("dp", "tp"))
    mat_spec = P(("dp", "tp"), None)
    return jax.shard_map(
        group_step,
        mesh=mesh,
        in_specs=(mat_spec, P(None), P(None), P("tp", None), P("tp"), row_spec, row_spec),
        out_specs=(row_spec, P("dp"), mat_spec, mat_spec, P("dp"), P("dp")),
        check_vma=False,
    )
```

```python
import functools

import jax
import jax.numpy as jnp
from jax import lax
from jax.experimental import pallas as pl
from jax.experimental.pallas import tpu as pltpu
from jax.sharding import PartitionSpec as P

SOFT_CAP = 30.0
Z_COEF = 1e-4
LN_EPS = 1e-5
EXP_SCALE = SOFT_CAP * 1.4426950408889634
MESH = pl.DeviceIdType.MESH
CHIPS = 4
OFFSET = (0, 1, 3, 2)
OWN, RIGHT, LEFT, OPP = range(4)
GRADS = ((0, OPP), (0, RIGHT), (0, LEFT), (0, OWN), (1, OPP), (1, RIGHT), (1, LEFT), (1, OWN))
HT = 128
CFG = (512, 512, 5, 8)
FS, FD, BS, DOT = 2048, 2048, 2048, 128
SLOTS = 6
LIM = 54 * 2**20
SUB = 32

TO_PARTNER, TO_RIGHT, TO_LEFT, FWD_RIGHT, FWD_LEFT, REL_LEFT, REL_RIGHT, REL_OPP_A, REL_OPP_B = range(9)
PAIR, OPP_RIGHT, OPP_LEFT, RIGHT_HI, RIGHT_LO, LEFT_LO, LEFT_HI = 0, 4, 5, 6, 7, 8, 9


def norm(h):
    mean = jnp.mean(h, axis=-1, keepdims=True)
    cent = h - mean
    rstd = lax.rsqrt(jnp.mean(cent * cent, axis=-1, keepdims=True) + LN_EPS)
    return cent * rstd, rstd


def kernel(
    hid_hbm, gain_hbm, bias_hbm, e_hbm, valid_hbm, tgt_hbm, msk_hbm,
    de, loss_out, dh_out, gain_out, bias_out,
    hid, gain, bias, valid, tgt, msk, in_sem,
    dz, x_all, w, xt, e, et, vb, tm_all, st_send, st_recv, av, dv, ls, dx, d2d, ring, fin, gb_send, gb_recv, iota,
    e_sem, tm_s, tm_r, ag_s, ag_r, st_s, st_r, rs_s, rs_r, gb_s, gb_r,
    *, vc, ec, n1, n2,
):
    group = 2 * CHIPS
    me = lax.axis_index("tp")
    c, k = me // 2, me % 2
    other = 1 - k
    partner = 2 * c + other
    chip = [(c + o) % CHIPS for o in OFFSET]
    right, left = 2 * chip[RIGHT] + k, 2 * chip[LEFT] + k
    vocab, dim = e_hbm.shape
    nv = vocab // vc

    def remote(src, dst, send, recv, dev):
        return pltpu.make_async_remote_copy(
            src_ref=src, dst_ref=dst, send_sem=send, recv_sem=recv, device_id={"tp": dev}, device_id_type=MESH
        )

    barrier = pltpu.get_barrier_semaphore()
    for j in range(1, group):
        pl.semaphore_signal(barrier, inc=1, device_id={"tp": (me + j) % group}, device_id_type=MESH)

    pairs = ((hid_hbm, hid), (gain_hbm, gain), (bias_hbm, bias), (tgt_hbm, tgt), (msk_hbm, msk), (valid_hbm, valid))
    inputs = [pltpu.make_async_copy(src, dst, in_sem.at[i]) for i, (src, dst) in enumerate(pairs)]
    for cp in inputs:
        cp.start()
    e_copies = [
        pltpu.make_async_copy(e_hbm.at[pl.ds(i * vc, vc)], e.at[pl.ds(i * vc, vc)], e_sem.at[i]) for i in range(nv)
    ]
    for cp in e_copies:
        cp.start()

    for cp in inputs[:5]:
        cp.wait()

    for h in range(2):
        xh, _ = norm(hid[h * HT : (h + 1) * HT, :].astype(jnp.float32))
        x_all[h, c, k] = (xh * gain[...] + bias[...]).astype(jnp.bfloat16)
    tm_all[me] = tgt[...] * 2 + msk[...]

    pl.semaphore_wait(barrier, group - 1)

    def ag(h, i, src, dst, dev):
        return remote(src, dst, ag_s.at[h * 9 + i], ag_r.at[h * 9 + i], dev)

    def lo(ref):
        return ref.at[pl.ds(0, HT // 2)]

    def hi(ref):
        return ref.at[pl.ds(HT // 2, HT // 2)]

    def block(h, r, core):
        return x_all.at[h, chip[r], core]

    def ag_copy(h, i):
        mine, lft, rgt, opp = block(h, OWN, k), block(h, LEFT, k), block(h, RIGHT, k), block(h, OPP, k)
        src, dev = {
            TO_PARTNER: (mine, partner),
            TO_RIGHT: (mine, right),
            TO_LEFT: (mine, left),
            FWD_RIGHT: (lo(lft), right),
            FWD_LEFT: (hi(rgt), left),
            REL_LEFT: (lft, partner),
            REL_RIGHT: (rgt, partner),
            REL_OPP_A: (lo(opp), partner),
            REL_OPP_B: (hi(opp), partner),
        }[i]
        return ag(h, i, src, src, dev)

    def ag_arrival(h, i):
        ref = {
            TO_PARTNER: block(h, OWN, other),
            TO_RIGHT: block(h, LEFT, k),
            TO_LEFT: block(h, RIGHT, k),
            FWD_RIGHT: lo(block(h, OPP, k)),
            FWD_LEFT: hi(block(h, OPP, k)),
            REL_LEFT: block(h, LEFT, other),
            REL_RIGHT: block(h, RIGHT, other),
            REL_OPP_A: lo(block(h, OPP, other)),
            REL_OPP_B: hi(block(h, OPP, other)),
        }[i]
        ag(h, i, ref, ref, partner).wait_recv()

    started = []

    def go(make, *args):
        make(*args).start()
        started.append((make, args))

    def tm_copy(j):
        return remote(tm_all.at[me], tm_all.at[me], tm_s.at[j - 1], tm_r.at[j - 1], (me + j) % group)

    for h in range(2):
        if h == 0:
            for j in range(1, group):
                go(tm_copy, j)
        for i in (TO_PARTNER, TO_RIGHT, TO_LEFT):
            go(ag_copy, h, i)

    def tm_arrival(j):
        ref = tm_all.at[(me - j + group) % group]
        remote(ref, ref, tm_s.at[j - 1], tm_r.at[j - 1], partner).wait_recv()

    inputs[5].wait()

    @pl.loop(0, vocab // 2048)
    def _(i):
        for u in range(16):
            row = jnp.broadcast_to(valid[pl.ds(i * 16 + u, 1), :].astype(jnp.float32), (128, 128))
            vb[pl.ds(pl.multiple_of(i * 2048 + u * 128, 128), 128), :] = row.T

    for cp in e_copies:
        cp.wait()

    iota[...] = lax.broadcasted_iota(jnp.int32, (SUB, 128), 0)

    def local_target(h, chip_no):
        halves = [
            jnp.broadcast_to((tm_all[2 * chip_no + kk, pl.ds(h, 1), :] >> 1) - me * vocab, (8, 128)) for kk in range(2)
        ]
        return jnp.concatenate(halves, axis=1)

    def weights(slot):
        return de.at[:, pl.ds(slot * 256, 256)] if slot < 2 else w.at[slot - 2]

    def fwd_begin(tiles):
        for n, (h, r, _) in enumerate(tiles):
            xt[:, n * 256 : (n + 1) * 256] = x_all[h, chip[r]].reshape(2 * HT, dim).T
        return [local_target(h, chip[r]) for h, r, _ in tiles]

    def softmax_part(rows0, size, tgts, tiles, carry):
        count = len(tiles)
        e_c = e.at[pl.ds(rows0, size)]
        vb_c = vb.at[pl.ds(rows0, size)]
        outs = [weights(slot).at[pl.ds(rows0, size)] for _, _, slot in tiles]
        carry = list(carry)
        for j in range(size // SUB):
            if j % (DOT // SUB) == 0:
                z = jnp.dot(
                    e_c[j * SUB : j * SUB + DOT, :], xt[:, : count * 256], preferred_element_type=jnp.float32
                )
            rows = slice(j * SUB, j * SUB + SUB)
            part = slice(j * SUB % DOT, j * SUB % DOT + SUB)
            ok, num = vb_c[rows, :], iota[...]
            ok = jnp.concatenate([ok, ok], axis=1)
            num = jnp.concatenate([num, num], axis=1).reshape(SUB // 8, 8, 256)
            for n in range(count):
                s_acc, t_acc = carry[n]
                t = jnp.tanh(z[part, n * 256 : (n + 1) * 256] * (1.0 / SOFT_CAP))
                ex = jnp.exp2(t * EXP_SCALE) * ok
                outs[n][rows, :] = ex * (1.0 - t * t)
                hit = num == (tgts[n] - (rows0 + j * SUB))[None]
                s_acc = s_acc + jnp.sum(ex.reshape(SUB // 8, 8, 256), axis=0)
                t_acc = jnp.where(hit, t.reshape(SUB // 8, 8, 256), t_acc)
                carry[n] = s_acc, t_acc
        return tuple(carry)

    def fwd_end(tiles, carry):
        for (h, r, _), (s_acc, t_acc) in zip(tiles, carry):
            s_row = jnp.sum(s_acc, axis=0, keepdims=True)
            t_row = jnp.sum(t_acc.reshape(SUB, 256), axis=0, keepdims=True)
            for kk in range(2):
                st_send[h, pl.ds(2 * chip[r] + kk, 1), :] = s_row[:, kk * 128 : (kk + 1) * 128]
                st_send[h, pl.ds(group + 2 * chip[r] + kk, 1), :] = t_row[:, kk * 128 : (kk + 1) * 128]

    def fwd_zero(tiles):
        zero = (jnp.zeros((8, 256), jnp.float32), jnp.zeros((SUB // 8, 8, 256), jnp.float32))
        return tuple(zero for _ in tiles)

    def forward(*tiles, halfway=None):
        size = FS if len(tiles) == 1 else FD
        steps = vocab // size
        tgts = fwd_begin(tiles)

        def body(i, carry):
            if halfway is not None:

                @pl.when(i == steps // 2)
                def _():
                    halfway()

            return softmax_part(pl.multiple_of(i * size, size), size, tgts, tiles, carry)

        fwd_end(tiles, lax.fori_loop(0, steps, body, fwd_zero(tiles)))

    def st_copy(h, j):
        n = h * (group - 1) + j - 1
        return remote(st_send.at[h], st_recv.at[h, j - 1], st_s.at[n], st_r.at[n], (me + j) % group)

    def stats_start(h):
        for j in range(1, group):
            go(st_copy, h, j)

    def token_count():
        total = jnp.zeros((2, 128), jnp.int32)
        for p in range(group):
            total = total + (tm_all[p] & 1)
        total = jnp.sum(jnp.sum(total.astype(jnp.float32), axis=1, keepdims=True), axis=0, keepdims=True)
        return total

    def stats_finish(h):
        tot = st_send[h]
        for j in range(1, group):
            st_copy(h, j).wait_recv()
        for j in range(1, group):
            tot = tot + st_recv[h, j - 1]
        s, t = tot[:group], tot[group:]
        mask = jnp.concatenate([tm_all[p, pl.ds(h, 1), :] & 1 for p in range(group)], axis=0).astype(jnp.float32)
        lse = jnp.log(s)
        coef = mask / token_count()
        a = (1.0 + 2.0 * Z_COEF * lse) * coef / s
        av[h] = a
        dv[h] = (a * jnp.exp2(t * EXP_SCALE) - coef) * (1.0 - t * t)
        ls[h] = (lse - SOFT_CAP * t + Z_COEF * lse * lse) * mask

    def spread(ref, h, chip_no):
        return jnp.concatenate(
            [jnp.broadcast_to(ref[h, pl.ds(2 * chip_no + kk, 1), :], (8, 128)) for kk in range(2)], axis=1
        )

    def bwd_begin(h, r):
        for kk in range(2):
            dx[h, r, kk] = jnp.zeros((dim, HT), jnp.float32)
        return local_target(h, chip[r]), spread(av, h, chip[r]), spread(dv, h, chip[r])

    def grad_store(h, r):
        n = GRADS.index((h, r))
        return dz.at[n] if n < 6 else e.at[:, pl.ds((n - 6) * 256, 256)]

    def hidden_part(i, size, h, r, slot, tgt8, a8, d8):
        rows0 = pl.multiple_of(i * size, size)
        w_c, dz_c = weights(slot).at[pl.ds(rows0, size)], grad_store(h, r).at[pl.ds(rows0, size)]
        part = None
        for u in range(size // vc):
            pieces = []
            for j in range(u * vc // SUB, (u + 1) * vc // SUB):
                rows = slice(j * SUB, j * SUB + SUB)
                num = iota[...]
                hit = jnp.concatenate([num, num], axis=1).reshape(SUB // 8, 8, 256) == (tgt8 - (rows0 + j * SUB))[None]
                g = jnp.where(hit, d8[None], a8[None] * w_c[rows, :].reshape(SUB // 8, 8, 256))
                g = g.reshape(SUB, 256).astype(jnp.bfloat16)
                dz_c[rows, :] = g
                pieces.append(g)
            more = jnp.dot(
                et[i * (size // vc) + u], jnp.concatenate(pieces, axis=0), preferred_element_type=jnp.float32
            )
            part = more if part is None else part + more
        return part

    def bwd_add(h, r, part):
        for kk in range(2):
            dx[h, r, kk] += part[:, kk * HT : (kk + 1) * HT]

    def backward(h, r, slot):
        vecs = bwd_begin(h, r)

        @pl.loop(0, vocab // BS)
        def _(i):
            bwd_add(h, r, hidden_part(i, BS, h, r, slot, *vecs))

    dlo, dhi = pl.ds(0, dim // 2), pl.ds(dim // 2, dim // 2)

    def rs(h, i, src, dst, dev):
        return remote(src, dst, rs_s.at[h * 10 + i], rs_r.at[h * 10 + i], dev)

    def pair_start(h, r):
        go(lambda: rs(h, PAIR + r, dx.at[h, r, other], d2d.at[h, r], partner))

    def pair_finish(h, r):
        rs(h, PAIR + r, d2d.at[h, r], d2d.at[h, r], partner).wait_recv()
        dx[h, r, k] = dx[h, r, k] + d2d[h, r]

    def opp_send(h):
        pair_finish(h, OPP)
        go(lambda: rs(h, OPP_RIGHT, dx.at[h, OPP, k, dlo], ring.at[h, 0], right))
        go(lambda: rs(h, OPP_LEFT, dx.at[h, OPP, k, dhi], ring.at[h, 1], left))

    def right_send(h):
        pair_finish(h, RIGHT)
        go(lambda: rs(h, RIGHT_HI, dx.at[h, RIGHT, k, dhi], fin.at[h, 0, dhi], right))

    def left_send(h):
        pair_finish(h, LEFT)
        go(lambda: rs(h, LEFT_LO, dx.at[h, LEFT, k, dlo], fin.at[h, 1, dlo], left))

    def ring_right(h):
        rs(h, OPP_RIGHT, ring.at[h, 0], ring.at[h, 0], partner).wait_recv()
        dx[h, RIGHT, k, dlo] = dx[h, RIGHT, k, dlo] + ring[h, 0]
        go(lambda: rs(h, RIGHT_LO, dx.at[h, RIGHT, k, dlo], fin.at[h, 0, dlo], right))

    def ring_left(h):
        rs(h, OPP_LEFT, ring.at[h, 1], ring.at[h, 1], partner).wait_recv()
        dx[h, LEFT, k, dhi] = dx[h, LEFT, k, dhi] + ring[h, 1]
        go(lambda: rs(h, LEFT_HI, dx.at[h, LEFT, k, dhi], fin.at[h, 1, dhi], left))

    def finish(h):
        for i, n, part in ((RIGHT_HI, 0, dhi), (RIGHT_LO, 0, dlo), (LEFT_LO, 1, dlo), (LEFT_HI, 1, dhi)):
            rs(h, i, fin.at[h, n, part], fin.at[h, n, part], partner).wait_recv()
        dn = (dx[h, OWN, k] + fin[h, 0] + fin[h, 1]).T
        xh, rstd = norm(hid[h * HT : (h + 1) * HT, :].astype(jnp.float32))
        dxh = dn * gain[...]
        m1 = jnp.mean(dxh, axis=-1, keepdims=True)
        m2 = jnp.mean(dxh * xh, axis=-1, keepdims=True)
        dh_out[h * HT : (h + 1) * HT, :] = (rstd * (dxh - m1 - xh * m2)).astype(jnp.bfloat16)
        return jnp.sum(dn * xh, axis=0, keepdims=True), jnp.sum(dn, axis=0, keepdims=True)

    def embed_rows(rows):
        acc = None
        for h in range(2):
            for r in range(CHIPS):
                xx = x_all[h, chip[r]].reshape(2 * HT, dim)
                part = jnp.dot(grad_store(h, r)[rows, :], xx, preferred_element_type=jnp.float32)
                acc = part if acc is None else acc + part
        return acc

    def embed(first, last):
        @pl.loop(first, last)
        def _(i):
            rows = pl.ds(pl.multiple_of(i * ec, ec), ec)
            de[rows, :] = embed_rows(rows)

    jp = 6 - 6 * k
    ref0 = tm_all.at[0]

    def ag_pass(h):
        ag_arrival(h, TO_RIGHT)
        ag_arrival(h, TO_LEFT)
        for i in (FWD_RIGHT, FWD_LEFT, REL_RIGHT, REL_LEFT):
            go(ag_copy, h, i)

    def ag_pass_opp(h):
        ag_arrival(h, FWD_RIGHT)
        ag_arrival(h, FWD_LEFT)
        for i in (REL_OPP_A, REL_OPP_B):
            go(ag_copy, h, i)

    remote(ref0, ref0, tm_s.at[jp], tm_r.at[jp], partner).wait_recv()
    ag_arrival(0, TO_PARTNER)
    ag_arrival(1, TO_PARTNER)
    forward((0, OWN, 0), (1, OWN, 1))
    for i in range(1, group - 1):
        n = (jp + i) % (group - 1)
        remote(ref0, ref0, tm_s.at[n], tm_r.at[n], partner).wait_recv()
    ag_pass(0)

    @pl.loop(0, nv // 4)
    def _(i):
        for u in range(4):
            et[i * 4 + u] = e[pl.ds(pl.multiple_of((i * 4 + u) * vc, vc), vc), :].T

    ag_arrival(0, REL_RIGHT)
    forward((0, RIGHT, 2))
    ag_pass(1)
    ag_pass_opp(0)
    ag_arrival(0, REL_LEFT)
    forward((0, LEFT, 3))
    ag_arrival(0, REL_OPP_A)
    ag_arrival(0, REL_OPP_B)
    forward((0, OPP, 4))
    stats_start(0)
    ag_pass_opp(1)
    ag_arrival(1, REL_RIGHT)
    forward((1, RIGHT, 5))
    stats_finish(0)
    ag_arrival(1, REL_LEFT)
    backward(0, OPP, 4)
    pair_start(0, OPP)
    backward(0, RIGHT, 2)
    pair_start(0, RIGHT)
    opp_send(0)
    ag_arrival(1, REL_OPP_A)
    ag_arrival(1, REL_OPP_B)
    forward((1, LEFT, 4), (1, OPP, 2), halfway=lambda: right_send(0))
    stats_start(1)
    backward(0, LEFT, 3)
    pair_start(0, LEFT)
    ring_right(0)
    backward(0, OWN, 0)
    pair_start(0, OWN)
    left_send(0)
    ring_left(0)
    stats_finish(1)
    for h in range(2):
        loss_out[h : h + 1, :] = ls[h, pl.ds(me, 1), :]
    total = ls[0] + ls[1]
    mean = jnp.sum(jnp.sum(total, axis=1, keepdims=True), axis=0, keepdims=True) / token_count()
    loss_out[2:, :] = jnp.broadcast_to(mean, (6, 128))
    backward(1, OPP, 2)
    pair_start(1, OPP)
    backward(1, RIGHT, 5)
    pair_start(1, RIGHT)
    opp_send(1)
    backward(1, LEFT, 4)
    pair_start(1, LEFT)
    right_send(1)
    backward(1, OWN, 1)
    pair_start(1, OWN)
    left_send(1)
    embed(0, 2)
    ring_right(1)
    ring_left(1)
    pair_finish(0, OWN)
    pair_finish(1, OWN)
    g0, b0 = finish(0)
    embed(2, n1)
    g1, b1 = finish(1)
    g, b = g0 + g1, b0 + b1
    for i in range(4):
        gb_send[i : i + 1, :] = g[:, i * 128 : (i + 1) * 128]
        gb_send[4 + i : 5 + i, :] = b[:, i * 128 : (i + 1) * 128]

    def gb_copy(j):
        return remote(gb_send, gb_recv.at[j - 1], gb_s.at[j - 1], gb_r.at[j - 1], (me + j) % group)

    for j in range(1, group):
        go(gb_copy, j)
    embed(n1, n2)
    tot = gb_send[...]
    for j in range(1, group):
        gb_copy(j).wait_recv()
        tot = tot + gb_recv[j - 1]
    gain_out[...], bias_out[...] = tot[:4], tot[4:]
    for make, args in started:
        make(*args).wait_send()


def write_out(
    de, loss_in, dh_in, gain_in, bias_in,
    loss_out, mean_out, dh_out, de_hbm, gain_out, bias_out,
    loss, mean, sems, *, pieces,
):
    rows = de_hbm.shape[0] // pieces
    copies = []

    def go(src, dst):
        copies.append(pltpu.make_async_copy(src, dst, sems.at[len(copies)]))
        copies[-1].start()

    for i in range(pieces):
        part = pl.ds(i * rows, rows)
        go(de.at[part], de_hbm.at[part])
    loss[...] = loss_in[0:2, :]
    mean[...] = loss_in[2:3, 0:1]
    for src, dst in ((dh_in, dh_out), (gain_in, gain_out), (bias_in, bias_out), (loss, loss_out), (mean, mean_out)):
        go(src, dst)
    for copy in copies:
        copy.wait()


def solution(mesh):
    assert mesh.shape["tp"] == 2 * CHIPS

    def group_step(hidden, ln_gain, ln_bias, out_embed, vocab_valid, targets, loss_mask):
        rows, dim = hidden.shape
        vocab = out_embed.shape[0]
        group = 2 * CHIPS
        assert rows == 2 * HT
        vc, ec, n1, n2 = CFG
        nv = vocab // vc
        f32, bf16, i32 = jnp.float32, jnp.bfloat16, jnp.int32
        vmem = pl.BlockSpec(memory_space=pltpu.VMEM)
        hbm = pl.BlockSpec(memory_space=pl.ANY)
        dma = pltpu.SemaphoreType.DMA
        results = pl.pallas_call(
            functools.partial(kernel, vc=vc, ec=ec, n1=n1, n2=n2),
            out_shape=(
                pltpu.VMEM((vocab, dim), f32),
                pltpu.VMEM((8, 128), f32),
                pltpu.VMEM((rows, dim), bf16),
                pltpu.VMEM((4, 128), f32),
                pltpu.VMEM((4, 128), f32),
            ),
            in_specs=[hbm] * 7,
            out_specs=(vmem,) * 5,
            scratch_shapes=[
                pltpu.VMEM((rows, dim), bf16),
                pltpu.VMEM((1, dim), f32),
                pltpu.VMEM((1, dim), f32),
                pltpu.VMEM((vocab // 128, 128), i32),
                pltpu.VMEM((2, 128), i32),
                pltpu.VMEM((2, 128), i32),
                dma((6,)),
                pltpu.VMEM((6, vocab, 2 * HT), bf16),
                pltpu.VMEM((2, CHIPS, 2, HT, dim), bf16),
                pltpu.VMEM((SLOTS - 2, vocab, 2 * HT), f32),
                pltpu.VMEM((dim, 4 * HT), bf16),
                pltpu.VMEM((vocab, dim), bf16),
                pltpu.VMEM((nv, dim, vc), bf16),
                pltpu.VMEM((vocab, 128), f32),
                pltpu.VMEM((group, 2, 128), i32),
                pltpu.VMEM((2, 2 * group, 128), f32),
                pltpu.VMEM((2, group - 1, 2 * group, 128), f32),
                pltpu.VMEM((2, group, 128), f32),
                pltpu.VMEM((2, group, 128), f32),
                pltpu.VMEM((2, group, 128), f32),
                pltpu.VMEM((2, CHIPS, 2, dim, HT), f32),
                pltpu.VMEM((2, CHIPS, dim, HT), f32),
                pltpu.VMEM((2, 2, dim // 2, HT), f32),
                pltpu.VMEM((2, 2, dim, HT), f32),
                pltpu.VMEM((8, 128), f32),
                pltpu.VMEM((group - 1, 8, 128), f32),
                pltpu.VMEM((SUB, 128), i32),
                dma((nv,)),
                dma((group - 1,)),
                dma((group - 1,)),
                dma((18,)),
                dma((18,)),
                dma((2 * (group - 1),)),
                dma((2 * (group - 1),)),
                dma((20,)),
                dma((20,)),
                dma((group - 1,)),
                dma((group - 1,)),
            ],
            compiler_params=pltpu.CompilerParams(
                collective_id=0, has_side_effects=True, vmem_limit_bytes=LIM
            ),
            name="vocab_xent",
        )(
            hidden,
            ln_gain.reshape(1, dim),
            ln_bias.reshape(1, dim),
            out_embed,
            vocab_valid.reshape(vocab // 128, 128),
            targets.reshape(2, 128),
            loss_mask.reshape(2, 128),
        )
        loss, mean, dh, de, dgain, dbias = pl.pallas_call(
            functools.partial(write_out, pieces=8),
            out_shape=(
                jax.ShapeDtypeStruct((2, 128), f32),
                jax.ShapeDtypeStruct((1, 1), f32),
                jax.ShapeDtypeStruct((rows, dim), bf16),
                jax.ShapeDtypeStruct((vocab, dim), f32),
                jax.ShapeDtypeStruct((4, 128), f32),
                jax.ShapeDtypeStruct((4, 128), f32),
            ),
            in_specs=[vmem] * 5,
            out_specs=(hbm,) * 6,
            scratch_shapes=[pltpu.VMEM((2, 128), f32), pltpu.VMEM((1, 1), f32), dma((13,))],
            compiler_params=pltpu.CompilerParams(vmem_limit_bytes=2 << 20),
            name="write_out",
        )(*results)
        return (
            loss.reshape(rows),
            mean.reshape(1),
            dh,
            de,
            dgain.reshape(dim),
            dbias.reshape(dim),
        )

    row_spec = P(("dp", "tp"))
    mat_spec = P(("dp", "tp"), None)
    return jax.shard_map(
        group_step,
        mesh=mesh,
        in_specs=(mat_spec, P(None), P(None), P("tp", None), P("tp"), row_spec, row_spec),
        out_specs=(row_spec, P("dp"), mat_spec, mat_spec, P("dp"), P("dp")),
        check_vma=False,
    )
```

```python
import functools

import jax
import jax.numpy as jnp
from jax import lax
from jax.experimental import pallas as pl
from jax.experimental.pallas import tpu as pltpu
from jax.sharding import PartitionSpec as P

SOFT_CAP = 30.0
Z_COEF = 1e-4
LN_EPS = 1e-5
EXP_SCALE = SOFT_CAP * 1.4426950408889634
MESH = pl.DeviceIdType.MESH
CHIPS = 4
OFFSET = (0, 1, 3, 2)
OWN, RIGHT, LEFT, OPP = range(4)
GRADS = ((0, OPP), (0, RIGHT), (0, LEFT), (0, OWN), (1, OPP), (1, RIGHT), (1, LEFT), (1, OWN))
HT = 128
CFG = (512, 512, 5, 8)
FS, FD, BS, DOT = 2048, 2048, 2048, 128
SLOTS = 6
LIM = 54 * 2**20
SUB = 32

TO_PARTNER, TO_RIGHT, TO_LEFT, FWD_RIGHT, FWD_LEFT, REL_LEFT, REL_RIGHT, REL_OPP_A, REL_OPP_B = range(9)
PAIR, OPP_RIGHT, OPP_LEFT, RIGHT_HI, RIGHT_LO, LEFT_LO, LEFT_HI = 0, 4, 5, 6, 7, 8, 9


def norm(h):
    mean = jnp.mean(h, axis=-1, keepdims=True)
    cent = h - mean
    rstd = lax.rsqrt(jnp.mean(cent * cent, axis=-1, keepdims=True) + LN_EPS)
    return cent * rstd, rstd


def kernel(
    hid_hbm, gain_hbm, bias_hbm, e_hbm, valid_hbm, tgt_hbm, msk_hbm,
    de, loss_out, dh_out, gain_out, bias_out,
    hid, gain, bias, valid, tgt, msk, in_sem,
    dz, x_all, w, xt, e, et, vb, tm_all, st_send, st_recv, av, dv, ls, dx, d2d, ring, fin, gb_send, gb_recv, iota,
    e_sem, tm_s, tm_r, ag_s, ag_r, st_s, st_r, rs_s, rs_r, gb_s, gb_r,
    *, vc, ec, n1, n2,
):
    group = 2 * CHIPS
    me = lax.axis_index("tp")
    c, k = me // 2, me % 2
    other = 1 - k
    partner = 2 * c + other
    chip = [(c + o) % CHIPS for o in OFFSET]
    right, left = 2 * chip[RIGHT] + k, 2 * chip[LEFT] + k
    vocab, dim = e_hbm.shape
    nv = vocab // vc

    def remote(src, dst, send, recv, dev):
        return pltpu.make_async_remote_copy(
            src_ref=src, dst_ref=dst, send_sem=send, recv_sem=recv, device_id={"tp": dev}, device_id_type=MESH
        )

    barrier = pltpu.get_barrier_semaphore()
    for j in range(1, group):
        pl.semaphore_signal(barrier, inc=1, device_id={"tp": (me + j) % group}, device_id_type=MESH)

    pairs = ((hid_hbm, hid), (gain_hbm, gain), (bias_hbm, bias), (tgt_hbm, tgt), (msk_hbm, msk), (valid_hbm, valid))
    inputs = [pltpu.make_async_copy(src, dst, in_sem.at[i]) for i, (src, dst) in enumerate(pairs)]
    for cp in inputs:
        cp.start()
    e_copies = [
        pltpu.make_async_copy(e_hbm.at[pl.ds(i * vc, vc)], e.at[pl.ds(i * vc, vc)], e_sem.at[i]) for i in range(nv)
    ]
    for cp in e_copies:
        cp.start()

    for cp in inputs[:5]:
        cp.wait()

    def normalize(h):
        xh, _ = norm(hid[h * HT : (h + 1) * HT, :].astype(jnp.float32))
        x_all[h, c, k] = (xh * gain[...] + bias[...]).astype(jnp.bfloat16)

    tm_all[me] = tgt[...] * 2 + msk[...]
    normalize(0)
    pl.semaphore_wait(barrier, group - 1)

    def ag(h, i, src, dst, dev):
        return remote(src, dst, ag_s.at[h * 9 + i], ag_r.at[h * 9 + i], dev)

    def lo(ref):
        return ref.at[pl.ds(0, HT // 2)]

    def hi(ref):
        return ref.at[pl.ds(HT // 2, HT // 2)]

    def block(h, r, core):
        return x_all.at[h, chip[r], core]

    def ag_copy(h, i):
        mine, lft, rgt, opp = block(h, OWN, k), block(h, LEFT, k), block(h, RIGHT, k), block(h, OPP, k)
        src, dev = {
            TO_PARTNER: (mine, partner),
            TO_RIGHT: (mine, right),
            TO_LEFT: (mine, left),
            FWD_RIGHT: (lo(lft), right),
            FWD_LEFT: (hi(rgt), left),
            REL_LEFT: (lft, partner),
            REL_RIGHT: (rgt, partner),
            REL_OPP_A: (lo(opp), partner),
            REL_OPP_B: (hi(opp), partner),
        }[i]
        return ag(h, i, src, src, dev)

    def ag_arrival(h, i):
        ref = {
            TO_PARTNER: block(h, OWN, other),
            TO_RIGHT: block(h, LEFT, k),
            TO_LEFT: block(h, RIGHT, k),
            FWD_RIGHT: lo(block(h, OPP, k)),
            FWD_LEFT: hi(block(h, OPP, k)),
            REL_LEFT: block(h, LEFT, other),
            REL_RIGHT: block(h, RIGHT, other),
            REL_OPP_A: lo(block(h, OPP, other)),
            REL_OPP_B: hi(block(h, OPP, other)),
        }[i]
        ag(h, i, ref, ref, partner).wait_recv()

    started = []

    def go(make, *args):
        make(*args).start()
        started.append((make, args))

    def tm_copy(j):
        return remote(tm_all.at[me], tm_all.at[me], tm_s.at[j - 1], tm_r.at[j - 1], (me + j) % group)

    for i in (TO_PARTNER, TO_RIGHT, TO_LEFT):
        go(ag_copy, 0, i)
    for j in range(1, group):
        go(tm_copy, j)
    normalize(1)
    for i in (TO_PARTNER, TO_RIGHT, TO_LEFT):
        go(ag_copy, 1, i)

    inputs[5].wait()

    @pl.loop(0, vocab // 2048)
    def _(i):
        for u in range(16):
            row = jnp.broadcast_to(valid[pl.ds(i * 16 + u, 1), :].astype(jnp.float32), (128, 128))
            vb[pl.ds(pl.multiple_of(i * 2048 + u * 128, 128), 128), :] = row.T

    for cp in e_copies:
        cp.wait()

    iota[...] = lax.broadcasted_iota(jnp.int32, (SUB, 128), 0)

    def local_target(h, chip_no):
        halves = [
            jnp.broadcast_to((tm_all[2 * chip_no + kk, pl.ds(h, 1), :] >> 1) - me * vocab, (8, 128)) for kk in range(2)
        ]
        return jnp.concatenate(halves, axis=1)

    def weights(slot):
        return de.at[:, pl.ds(slot * 256, 256)] if slot < 2 else w.at[slot - 2]

    def fwd_begin(tiles):
        for n, (h, r, _) in enumerate(tiles):
            xt[:, n * 256 : (n + 1) * 256] = x_all[h, chip[r]].reshape(2 * HT, dim).T
        return [local_target(h, chip[r]) for h, r, _ in tiles]

    def softmax_part(rows0, size, tgts, tiles, carry):
        count = len(tiles)
        e_c = e.at[pl.ds(rows0, size)]
        vb_c = vb.at[pl.ds(rows0, size)]
        outs = [weights(slot).at[pl.ds(rows0, size)] for _, _, slot in tiles]
        carry = list(carry)
        for j in range(size // SUB):
            if j % (DOT // SUB) == 0:
                z = jnp.dot(
                    e_c[j * SUB : j * SUB + DOT, :], xt[:, : count * 256], preferred_element_type=jnp.float32
                )
            rows = slice(j * SUB, j * SUB + SUB)
            part = slice(j * SUB % DOT, j * SUB % DOT + SUB)
            ok, num = vb_c[rows, :], iota[...]
            ok = jnp.concatenate([ok, ok], axis=1)
            num = jnp.concatenate([num, num], axis=1).reshape(SUB // 8, 8, 256)
            for n in range(count):
                s_acc, t_acc = carry[n]
                t = jnp.tanh(z[part, n * 256 : (n + 1) * 256] * (1.0 / SOFT_CAP))
                ex = jnp.exp2(t * EXP_SCALE) * ok
                outs[n][rows, :] = ex * (1.0 - t * t)
                hit = num == (tgts[n] - (rows0 + j * SUB))[None]
                s_acc = s_acc + jnp.sum(ex.reshape(SUB // 8, 8, 256), axis=0)
                t_acc = jnp.where(hit, t.reshape(SUB // 8, 8, 256), t_acc)
                carry[n] = s_acc, t_acc
        return tuple(carry)

    def fwd_end(tiles, carry):
        for (h, r, _), (s_acc, t_acc) in zip(tiles, carry):
            s_row = jnp.sum(s_acc, axis=0, keepdims=True)
            t_row = jnp.sum(t_acc.reshape(SUB, 256), axis=0, keepdims=True)
            for kk in range(2):
                st_send[h, pl.ds(2 * chip[r] + kk, 1), :] = s_row[:, kk * 128 : (kk + 1) * 128]
                st_send[h, pl.ds(group + 2 * chip[r] + kk, 1), :] = t_row[:, kk * 128 : (kk + 1) * 128]

    def fwd_zero(tiles):
        zero = (jnp.zeros((8, 256), jnp.float32), jnp.zeros((SUB // 8, 8, 256), jnp.float32))
        return tuple(zero for _ in tiles)

    def forward(*tiles, halfway=None):
        size = FS if len(tiles) == 1 else FD
        steps = vocab // size
        tgts = fwd_begin(tiles)

        def body(i, carry):
            if halfway is not None:

                @pl.when(i == steps // 2)
                def _():
                    halfway()

            return softmax_part(pl.multiple_of(i * size, size), size, tgts, tiles, carry)

        fwd_end(tiles, lax.fori_loop(0, steps, body, fwd_zero(tiles)))

    def st_copy(h, j):
        n = h * (group - 1) + j - 1
        return remote(st_send.at[h], st_recv.at[h, j - 1], st_s.at[n], st_r.at[n], (me + j) % group)

    def stats_start(h):
        for j in range(1, group):
            go(st_copy, h, j)

    def token_count():
        total = jnp.zeros((2, 128), jnp.int32)
        for p in range(group):
            total = total + (tm_all[p] & 1)
        total = jnp.sum(jnp.sum(total.astype(jnp.float32), axis=1, keepdims=True), axis=0, keepdims=True)
        return total

    def stats_finish(h):
        tot = st_send[h]
        for j in range(1, group):
            st_copy(h, j).wait_recv()
        for j in range(1, group):
            tot = tot + st_recv[h, j - 1]
        s, t = tot[:group], tot[group:]
        mask = jnp.concatenate([tm_all[p, pl.ds(h, 1), :] & 1 for p in range(group)], axis=0).astype(jnp.float32)
        lse = jnp.log(s)
        coef = mask / token_count()
        a = (1.0 + 2.0 * Z_COEF * lse) * coef / s
        av[h] = a
        dv[h] = (a * jnp.exp2(t * EXP_SCALE) - coef) * (1.0 - t * t)
        ls[h] = (lse - SOFT_CAP * t + Z_COEF * lse * lse) * mask

    def spread(ref, h, chip_no):
        return jnp.concatenate(
            [jnp.broadcast_to(ref[h, pl.ds(2 * chip_no + kk, 1), :], (8, 128)) for kk in range(2)], axis=1
        )

    def bwd_begin(h, r):
        for kk in range(2):
            dx[h, r, kk] = jnp.zeros((dim, HT), jnp.float32)
        return local_target(h, chip[r]), spread(av, h, chip[r]), spread(dv, h, chip[r])

    def grad_store(h, r):
        n = GRADS.index((h, r))
        return dz.at[n] if n < 6 else e.at[:, pl.ds((n - 6) * 256, 256)]

    def hidden_part(i, size, h, r, slot, tgt8, a8, d8):
        rows0 = pl.multiple_of(i * size, size)
        w_c, dz_c = weights(slot).at[pl.ds(rows0, size)], grad_store(h, r).at[pl.ds(rows0, size)]
        part = None
        for u in range(size // vc):
            pieces = []
            for j in range(u * vc // SUB, (u + 1) * vc // SUB):
                rows = slice(j * SUB, j * SUB + SUB)
                num = iota[...]
                hit = jnp.concatenate([num, num], axis=1).reshape(SUB // 8, 8, 256) == (tgt8 - (rows0 + j * SUB))[None]
                g = jnp.where(hit, d8[None], a8[None] * w_c[rows, :].reshape(SUB // 8, 8, 256))
                g = g.reshape(SUB, 256).astype(jnp.bfloat16)
                dz_c[rows, :] = g
                pieces.append(g)
            more = jnp.dot(
                et[i * (size // vc) + u], jnp.concatenate(pieces, axis=0), preferred_element_type=jnp.float32
            )
            part = more if part is None else part + more
        return part

    def bwd_add(h, r, part):
        for kk in range(2):
            dx[h, r, kk] += part[:, kk * HT : (kk + 1) * HT]

    def backward(h, r, slot):
        vecs = bwd_begin(h, r)

        @pl.loop(0, vocab // BS)
        def _(i):
            bwd_add(h, r, hidden_part(i, BS, h, r, slot, *vecs))

    dlo, dhi = pl.ds(0, dim // 2), pl.ds(dim // 2, dim // 2)

    def rs(h, i, src, dst, dev):
        return remote(src, dst, rs_s.at[h * 10 + i], rs_r.at[h * 10 + i], dev)

    def pair_start(h, r):
        go(lambda: rs(h, PAIR + r, dx.at[h, r, other], d2d.at[h, r], partner))

    def pair_finish(h, r):
        rs(h, PAIR + r, d2d.at[h, r], d2d.at[h, r], partner).wait_recv()
        dx[h, r, k] = dx[h, r, k] + d2d[h, r]

    def opp_send(h):
        pair_finish(h, OPP)
        go(lambda: rs(h, OPP_RIGHT, dx.at[h, OPP, k, dlo], ring.at[h, 0], right))
        go(lambda: rs(h, OPP_LEFT, dx.at[h, OPP, k, dhi], ring.at[h, 1], left))

    def right_send(h):
        pair_finish(h, RIGHT)
        go(lambda: rs(h, RIGHT_HI, dx.at[h, RIGHT, k, dhi], fin.at[h, 0, dhi], right))

    def left_send(h):
        pair_finish(h, LEFT)
        go(lambda: rs(h, LEFT_LO, dx.at[h, LEFT, k, dlo], fin.at[h, 1, dlo], left))

    def ring_right(h):
        rs(h, OPP_RIGHT, ring.at[h, 0], ring.at[h, 0], partner).wait_recv()
        dx[h, RIGHT, k, dlo] = dx[h, RIGHT, k, dlo] + ring[h, 0]
        go(lambda: rs(h, RIGHT_LO, dx.at[h, RIGHT, k, dlo], fin.at[h, 0, dlo], right))

    def ring_left(h):
        rs(h, OPP_LEFT, ring.at[h, 1], ring.at[h, 1], partner).wait_recv()
        dx[h, LEFT, k, dhi] = dx[h, LEFT, k, dhi] + ring[h, 1]
        go(lambda: rs(h, LEFT_HI, dx.at[h, LEFT, k, dhi], fin.at[h, 1, dhi], left))

    def finish(h):
        for i, n, part in ((RIGHT_HI, 0, dhi), (RIGHT_LO, 0, dlo), (LEFT_LO, 1, dlo), (LEFT_HI, 1, dhi)):
            rs(h, i, fin.at[h, n, part], fin.at[h, n, part], partner).wait_recv()
        dn = (dx[h, OWN, k] + fin[h, 0] + fin[h, 1]).T
        xh, rstd = norm(hid[h * HT : (h + 1) * HT, :].astype(jnp.float32))
        dxh = dn * gain[...]
        m1 = jnp.mean(dxh, axis=-1, keepdims=True)
        m2 = jnp.mean(dxh * xh, axis=-1, keepdims=True)
        dh_out[h * HT : (h + 1) * HT, :] = (rstd * (dxh - m1 - xh * m2)).astype(jnp.bfloat16)
        return jnp.sum(dn * xh, axis=0, keepdims=True), jnp.sum(dn, axis=0, keepdims=True)

    def embed_rows(rows):
        acc = None
        for h in range(2):
            for r in range(CHIPS):
                xx = x_all[h, chip[r]].reshape(2 * HT, dim)
                part = jnp.dot(grad_store(h, r)[rows, :], xx, preferred_element_type=jnp.float32)
                acc = part if acc is None else acc + part
        return acc

    def embed(first, last):
        @pl.loop(first, last)
        def _(i):
            rows = pl.ds(pl.multiple_of(i * ec, ec), ec)
            de[rows, :] = embed_rows(rows)

    jp = 6 - 6 * k
    ref0 = tm_all.at[0]

    def ag_pass(h):
        ag_arrival(h, TO_RIGHT)
        ag_arrival(h, TO_LEFT)
        for i in (FWD_RIGHT, FWD_LEFT, REL_RIGHT, REL_LEFT):
            go(ag_copy, h, i)

    def ag_pass_opp(h):
        ag_arrival(h, FWD_RIGHT)
        ag_arrival(h, FWD_LEFT)
        for i in (REL_OPP_A, REL_OPP_B):
            go(ag_copy, h, i)

    remote(ref0, ref0, tm_s.at[jp], tm_r.at[jp], partner).wait_recv()
    ag_arrival(0, TO_PARTNER)
    ag_arrival(1, TO_PARTNER)
    forward((0, OWN, 0), (1, OWN, 1))
    for i in range(1, group - 1):
        n = (jp + i) % (group - 1)
        remote(ref0, ref0, tm_s.at[n], tm_r.at[n], partner).wait_recv()
    ag_pass(0)

    @pl.loop(0, nv // 4)
    def _(i):
        for u in range(4):
            et[i * 4 + u] = e[pl.ds(pl.multiple_of((i * 4 + u) * vc, vc), vc), :].T

    ag_arrival(0, REL_RIGHT)
    forward((0, RIGHT, 2))
    ag_pass(1)
    ag_pass_opp(0)
    ag_arrival(0, REL_LEFT)
    forward((0, LEFT, 3))
    ag_arrival(0, REL_OPP_A)
    ag_arrival(0, REL_OPP_B)
    forward((0, OPP, 4))
    stats_start(0)
    ag_pass_opp(1)
    ag_arrival(1, REL_RIGHT)
    forward((1, RIGHT, 5))
    stats_finish(0)
    ag_arrival(1, REL_LEFT)
    backward(0, OPP, 4)
    pair_start(0, OPP)
    backward(0, RIGHT, 2)
    pair_start(0, RIGHT)
    opp_send(0)
    ag_arrival(1, REL_OPP_A)
    ag_arrival(1, REL_OPP_B)
    forward((1, LEFT, 4), (1, OPP, 2), halfway=lambda: right_send(0))
    stats_start(1)
    backward(0, LEFT, 3)
    pair_start(0, LEFT)
    ring_right(0)
    backward(0, OWN, 0)
    pair_start(0, OWN)
    left_send(0)
    ring_left(0)
    stats_finish(1)
    for h in range(2):
        loss_out[h : h + 1, :] = ls[h, pl.ds(me, 1), :]
    total = ls[0] + ls[1]
    mean = jnp.sum(jnp.sum(total, axis=1, keepdims=True), axis=0, keepdims=True) / token_count()
    loss_out[2:, :] = jnp.broadcast_to(mean, (6, 128))
    backward(1, OPP, 2)
    pair_start(1, OPP)
    backward(1, RIGHT, 5)
    pair_start(1, RIGHT)
    opp_send(1)
    backward(1, LEFT, 4)
    pair_start(1, LEFT)
    right_send(1)
    backward(1, OWN, 1)
    pair_start(1, OWN)
    left_send(1)
    embed(0, 2)
    ring_right(1)
    ring_left(1)
    pair_finish(0, OWN)
    pair_finish(1, OWN)
    g0, b0 = finish(0)
    embed(2, n1)
    g1, b1 = finish(1)
    g, b = g0 + g1, b0 + b1
    for i in range(4):
        gb_send[i : i + 1, :] = g[:, i * 128 : (i + 1) * 128]
        gb_send[4 + i : 5 + i, :] = b[:, i * 128 : (i + 1) * 128]

    def gb_copy(j):
        return remote(gb_send, gb_recv.at[j - 1], gb_s.at[j - 1], gb_r.at[j - 1], (me + j) % group)

    for j in range(1, group):
        go(gb_copy, j)
    embed(n1, n2)
    tot = gb_send[...]
    for j in range(1, group):
        gb_copy(j).wait_recv()
        tot = tot + gb_recv[j - 1]
    gain_out[...], bias_out[...] = tot[:4], tot[4:]
    for make, args in started:
        make(*args).wait_send()


def write_out(
    de, loss_in, dh_in, gain_in, bias_in,
    loss_out, mean_out, dh_out, de_hbm, gain_out, bias_out,
    loss, mean, sems, *, pieces,
):
    rows = de_hbm.shape[0] // pieces
    copies = []

    def go(src, dst):
        copies.append(pltpu.make_async_copy(src, dst, sems.at[len(copies)]))
        copies[-1].start()

    for i in range(pieces):
        part = pl.ds(i * rows, rows)
        go(de.at[part], de_hbm.at[part])
    loss[...] = loss_in[0:2, :]
    mean[...] = loss_in[2:3, 0:1]
    for src, dst in ((dh_in, dh_out), (gain_in, gain_out), (bias_in, bias_out), (loss, loss_out), (mean, mean_out)):
        go(src, dst)
    for copy in copies:
        copy.wait()


def solution(mesh):
    assert mesh.shape["tp"] == 2 * CHIPS

    def group_step(hidden, ln_gain, ln_bias, out_embed, vocab_valid, targets, loss_mask):
        rows, dim = hidden.shape
        vocab = out_embed.shape[0]
        group = 2 * CHIPS
        assert rows == 2 * HT
        vc, ec, n1, n2 = CFG
        nv = vocab // vc
        f32, bf16, i32 = jnp.float32, jnp.bfloat16, jnp.int32
        vmem = pl.BlockSpec(memory_space=pltpu.VMEM)
        hbm = pl.BlockSpec(memory_space=pl.ANY)
        dma = pltpu.SemaphoreType.DMA
        results = pl.pallas_call(
            functools.partial(kernel, vc=vc, ec=ec, n1=n1, n2=n2),
            out_shape=(
                pltpu.VMEM((vocab, dim), f32),
                pltpu.VMEM((8, 128), f32),
                pltpu.VMEM((rows, dim), bf16),
                pltpu.VMEM((4, 128), f32),
                pltpu.VMEM((4, 128), f32),
            ),
            in_specs=[hbm] * 7,
            out_specs=(vmem,) * 5,
            scratch_shapes=[
                pltpu.VMEM((rows, dim), bf16),
                pltpu.VMEM((1, dim), f32),
                pltpu.VMEM((1, dim), f32),
                pltpu.VMEM((vocab // 128, 128), i32),
                pltpu.VMEM((2, 128), i32),
                pltpu.VMEM((2, 128), i32),
                dma((6,)),
                pltpu.VMEM((6, vocab, 2 * HT), bf16),
                pltpu.VMEM((2, CHIPS, 2, HT, dim), bf16),
                pltpu.VMEM((SLOTS - 2, vocab, 2 * HT), f32),
                pltpu.VMEM((dim, 4 * HT), bf16),
                pltpu.VMEM((vocab, dim), bf16),
                pltpu.VMEM((nv, dim, vc), bf16),
                pltpu.VMEM((vocab, 128), f32),
                pltpu.VMEM((group, 2, 128), i32),
                pltpu.VMEM((2, 2 * group, 128), f32),
                pltpu.VMEM((2, group - 1, 2 * group, 128), f32),
                pltpu.VMEM((2, group, 128), f32),
                pltpu.VMEM((2, group, 128), f32),
                pltpu.VMEM((2, group, 128), f32),
                pltpu.VMEM((2, CHIPS, 2, dim, HT), f32),
                pltpu.VMEM((2, CHIPS, dim, HT), f32),
                pltpu.VMEM((2, 2, dim // 2, HT), f32),
                pltpu.VMEM((2, 2, dim, HT), f32),
                pltpu.VMEM((8, 128), f32),
                pltpu.VMEM((group - 1, 8, 128), f32),
                pltpu.VMEM((SUB, 128), i32),
                dma((nv,)),
                dma((group - 1,)),
                dma((group - 1,)),
                dma((18,)),
                dma((18,)),
                dma((2 * (group - 1),)),
                dma((2 * (group - 1),)),
                dma((20,)),
                dma((20,)),
                dma((group - 1,)),
                dma((group - 1,)),
            ],
            compiler_params=pltpu.CompilerParams(
                collective_id=0, has_side_effects=True, vmem_limit_bytes=LIM
            ),
            name="vocab_xent",
        )(
            hidden,
            ln_gain.reshape(1, dim),
            ln_bias.reshape(1, dim),
            out_embed,
            vocab_valid.reshape(vocab // 128, 128),
            targets.reshape(2, 128),
            loss_mask.reshape(2, 128),
        )
        loss, mean, dh, de, dgain, dbias = pl.pallas_call(
            functools.partial(write_out, pieces=8),
            out_shape=(
                jax.ShapeDtypeStruct((2, 128), f32),
                jax.ShapeDtypeStruct((1, 1), f32),
                jax.ShapeDtypeStruct((rows, dim), bf16),
                jax.ShapeDtypeStruct((vocab, dim), f32),
                jax.ShapeDtypeStruct((4, 128), f32),
                jax.ShapeDtypeStruct((4, 128), f32),
            ),
            in_specs=[vmem] * 5,
            out_specs=(hbm,) * 6,
            scratch_shapes=[pltpu.VMEM((2, 128), f32), pltpu.VMEM((1, 1), f32), dma((13,))],
            compiler_params=pltpu.CompilerParams(vmem_limit_bytes=2 << 20),
            name="write_out",
        )(*results)
        return (
            loss.reshape(rows),
            mean.reshape(1),
            dh,
            de,
            dgain.reshape(dim),
            dbias.reshape(dim),
        )

    row_spec = P(("dp", "tp"))
    mat_spec = P(("dp", "tp"), None)
    return jax.shard_map(
        group_step,
        mesh=mesh,
        in_specs=(mat_spec, P(None), P(None), P("tp", None), P("tp"), row_spec, row_spec),
        out_specs=(row_spec, P("dp"), mat_spec, mat_spec, P("dp"), P("dp")),
        check_vma=False,
    )
```
